256 devices in a mesh: img: 16 (over y, x), row: 16 (over z, core).
Axes of the slice: x: 4, y: 4, z: 8, core: 2. Of those that a mesh axis runs over, the one named last changes fastest.
Arguments:
- latent: bfloat16 [1024, 128, 512], P(('img', 'row')), parts along dimension 0, may hold values from -8 to 8
- attn_gain: float32 [512], replicated, may hold values from 0.5 to 1.5
- attn_shift: float32 [512], replicated, may hold values from -3 to 3
- w_query: bfloat16 [512, 512], replicated, may hold values from -2 to 2
- w_key: bfloat16 [512, 512], replicated, may hold values from -2 to 2
- w_value: bfloat16 [512, 512], replicated, may hold values from -0.25 to 0.25
- w_out: bfloat16 [512, 512], replicated, may hold values from -0.25 to 0.25
- conv_gain: float32 [512], replicated, may hold values from 0.5 to 1.5
- conv_shift: float32 [512], replicated, may hold values from -3 to 3
- w_conv: bfloat16 [3, 3, 512, 512], replicated, may hold values from -0.09375 to 0.09375
- conv_bias: float32 [512], replicated, may hold values from -3 to 3
Outputs:
- encoded: bfloat16 [1024, 128, 512], P(('img', 'row')), parts along dimension 0
The draws below stay inside these ranges and needn't reach their ends.
There are 16 independent parts, one for each index of `img`. The reference program is written for one: setup_inputs(seed, part) draws one part's arguments, and reference() takes and returns one part's arrays. A program takes and returns all parts, laid end to end along the dimension named above; an argument that names none is the same for every part. Nothing has to cross between parts.
All inputs are finite; a program needn't handle non-finite values.
Results may differ from the reference program's by a relative error of at most 0.011.
Values may be sent and summed in bfloat16 or wider, within the bound.
A program may use at most 128 MiB of HBM per device.

```python
import jax
import jax.numpy as jnp
from jax import lax

C = 512
GROUPS = 32
W = 128
H = 64


def shared_gauss(key):
    return jnp.clip(jax.random.normal(jax.random.fold_in(key, 7), (C, C), jnp.float32), -3.0, 3.0)


def draw_latent(key, part):
    noise = jax.random.normal(jax.random.fold_in(key, 3), (H, W, C), jnp.float32)
    rows = (jnp.arange(H, dtype=jnp.float32) + 0.5) / H
    phase = jax.random.uniform(jax.random.fold_in(key, 13), (GROUPS,), jnp.float32, -jnp.pi, jnp.pi)
    amplitude = jax.random.uniform(jax.random.fold_in(key, 17), (C,), jnp.float32, 0.8, 1.6)
    wave = jnp.sin(2.0 * jnp.pi * rows[:, None] + phase[None, :])
    offset = jnp.repeat(wave, C // GROUPS, axis=1) * amplitude[None, :]
    result = noise + offset[:, None, :]
    return jnp.clip(result, -8.0, 8.0).astype(jnp.bfloat16)


def draw_w_query(key, part):
    return (shared_gauss(key) * (4.0 / jnp.sqrt(jnp.float32(C)))).astype(jnp.bfloat16)


def draw_w_key(key, part):
    fresh = jnp.clip(jax.random.normal(jax.random.fold_in(key, 11), (C, C), jnp.float32), -3.0, 3.0)
    result = fresh / jnp.sqrt(jnp.float32(C))
    return result.astype(jnp.bfloat16)


def scatter_about(stream_key, extent, scale, most, kind=jnp.bfloat16):
    return jnp.clip(scale * jax.random.normal(stream_key, extent, jnp.float32), -most, most).astype(kind)


def setup_inputs(seed: int = 0, part: int = 0) -> dict:
    key_list = jax.random.split(jax.random.key(seed), 12)
    part_splits = jax.random.split(jax.random.fold_in(key_list[11], part), 12)
    return {
        "latent": draw_latent(jax.random.fold_in(jax.random.fold_in(key_list[11], part), 71), part),
        "attn_gain": jnp.clip(1.0 + 0.1 * jax.random.normal(key_list[1], (C,), jnp.float32), 0.5, 1.5),
        "attn_shift": scatter_about(key_list[2], (C,), 0.5, 3.0, jnp.float32),
        "w_query": draw_w_query(jax.random.fold_in(key_list[11], 71), part),
        "w_key": draw_w_key(jax.random.fold_in(key_list[11], 71), part),
        "w_value": scatter_about(key_list[5], (C, C), C ** -0.5, 0.25),
        "w_out": scatter_about(key_list[6], (C, C), C ** -0.5, 0.25),
        "conv_gain": jnp.clip(1.0 + 0.1 * jax.random.normal(key_list[7], (C,), jnp.float32), 0.5, 1.5),
        "conv_shift": scatter_about(key_list[8], (C,), 0.5, 3.0, jnp.float32),
        "w_conv": scatter_about(key_list[9], (3, 3, C, C), (9 * C) ** -0.5, 0.09375),
        "conv_bias": scatter_about(key_list[10], (C,), 0.5, 3.0, jnp.float32),
    }


epsilon = 1e-06

def group_norm(field, gain, shift):
    grouped = field.astype(jnp.float32).reshape(field.shape[0], GROUPS, C // GROUPS)
    centre = lax.optimization_barrier(jnp.mean(grouped, axis=(0, 2)))
    offset = grouped - centre[None, :, None]
    spread = lax.optimization_barrier(jnp.mean(offset * offset, axis=(0, 2)))
    normed = offset * lax.rsqrt(spread + epsilon)[None, :, None]
    return normed.reshape(field.shape) * gain + shift

def reference(latent, attn_gain, attn_shift, w_query, w_key, w_value, w_out, conv_gain, conv_shift, w_conv, conv_bias):
    positions = latent.reshape(H * W, C)
    normed = group_norm(positions, attn_gain, attn_shift).astype(jnp.bfloat16)
    queries = jnp.dot(normed, w_query, preferred_element_type=jnp.float32).astype(jnp.bfloat16)
    key_rows = jnp.dot(normed, w_key, preferred_element_type=jnp.float32).astype(jnp.bfloat16)
    values = jnp.dot(normed, w_value, preferred_element_type=jnp.float32).astype(jnp.bfloat16)
    scaling = 1.0 / jnp.sqrt(jnp.float32(C))
    scores = jnp.einsum('qc,kc->qk', queries.astype(jnp.float32), key_rows.astype(jnp.float32)) * scaling
    rowmax = lax.optimization_barrier(jnp.max(scores, axis=1))
    expo = jnp.exp(scores - rowmax[:, None])
    denominator = lax.optimization_barrier(jnp.sum(expo, axis=1))
    probs = expo.astype(jnp.bfloat16)
    attended = (jnp.dot(probs, values, preferred_element_type=jnp.float32) / denominator[:, None]).astype(jnp.bfloat16)
    hidden = (positions.astype(jnp.float32) + jnp.dot(attended, w_out, preferred_element_type=jnp.float32)).astype(jnp.bfloat16)
    activated = jax.nn.silu(group_norm(hidden, conv_gain, conv_shift)).astype(jnp.bfloat16).reshape(H, W, C)
    padded = jnp.pad(activated, ((1, 1), (1, 1), (0, 0)))
    convolved = jnp.zeros((H * W, C), jnp.float32)
    for row_tap in range(3):
        for col_tap in range(3):
            window = padded[row_tap:row_tap + H, col_tap:col_tap + W].reshape(H * W, C)
            convolved = convolved + jnp.dot(window, w_conv[row_tap, col_tap], preferred_element_type=jnp.float32)
    encoded = hidden.astype(jnp.float32) + (convolved + conv_bias)
    return encoded.astype(jnp.bfloat16).reshape(H, W, C)
```

```python
import functools

import jax
import jax.numpy as jnp
from jax import lax
from jax.experimental import pallas as pl
from jax.experimental.pallas import tpu as pltpu
from jax.sharding import PartitionSpec as P

MESH = pl.DeviceIdType.MESH
C = 512
GROUP = 16
W = 128
EPS = 1e-06
PIECE = 128
LOG2E = 1.4426950408889634
F32 = jnp.float32
BF16 = jnp.bfloat16


def group_total(x):
    lane = lax.broadcasted_iota(jnp.int32, x.shape, 1)
    width = x.shape[1]
    for s in (1, 2, 4, 8):
        up = pltpu.roll(x, s, 1)
        down = pltpu.roll(x, width - s, 1)
        x = x + jnp.where((lane // s) % 2 == 1, up, down)
    return x


def channel_stats(x):
    mean = jnp.sum(x, axis=0, keepdims=True) * (1.0 / x.shape[0])
    off = x - mean
    return mean, jnp.sum(off * off, axis=0, keepdims=True)


def affine(means, seconds, count, gain, shift):
    devices = means.shape[0]
    centre = group_total(
        jnp.broadcast_to(jnp.sum(means, axis=0, keepdims=True), (8, C))
    )[:1] * (1.0 / (devices * GROUP))
    off = means - centre
    second = jnp.sum(seconds + count * (off * off), axis=0, keepdims=True)
    spread = group_total(jnp.broadcast_to(second, (8, C)))[:1] * (1.0 / (devices * GROUP * count))
    a = lax.rsqrt(spread + EPS) * gain
    return a, shift - centre * a


def dot(x, y):
    return jnp.dot(x, y, preferred_element_type=F32)


def dot_t(x, y):
    return lax.dot_general(x, y, (((1,), (1,)), ((), ())), preferred_element_type=F32)


def kernel(
    n,
    lat,
    vecs,
    wq,
    wk,
    wv,
    wo,
    wc,
    out,
    gathered,
    vec,
    wq_v,
    wk_v,
    wv_v,
    wo_v,
    wc_v,
    q_v,
    m_v,
    l_v,
    acc_v,
    hid_v,
    halo_v,
    act_v,
    st1,
    st2,
    local_sem,
    ring_send,
    ring_recv,
    sib_send,
    sib_recv,
    st_send,
    st_recv,
    halo_send,
    halo_recv,
):
    me = lax.axis_index("row")
    chips = n // 2
    z, core = me // 2, me % 2
    sib = me + 1 - 2 * core
    count = lat.shape[0]
    parts = count // PIECE
    half = chips // 2
    steps = (half - 1) * parts + parts // 2
    nexts = (
        lax.rem(z + 1, chips) * 2 + core,
        lax.rem(z + chips - 1, chips) * 2 + core,
    )

    get_lat = pltpu.make_async_copy(lat, gathered.at[me], local_sem.at[0])
    get_lat.start()
    get_vec = pltpu.make_async_copy(vecs, vec, local_sem.at[1])
    get_vec.start()
    gets = []
    for i, (a, b) in enumerate(((wq, wq_v), (wk, wk_v), (wv, wv_v), (wo, wo_v), (wc, wc_v))):
        gets.append(pltpu.make_async_copy(a, b, local_sem.at[2 + i]))
        gets[-1].start()

    barrier = pltpu.get_barrier_semaphore()
    for k in range(1, n):
        pl.semaphore_signal(
            barrier, inc=1, device_id={"row": lax.rem(me + k, n)}, device_id_type=MESH
        )
    pl.semaphore_wait(barrier, n - 1)

    def place(d, r, c):
        hop = 1 + r // parts
        chip = lax.rem(z + chips - hop, chips) if d == 0 else lax.rem(z + hop, chips)
        j = lax.rem(r, parts) if d == 0 else lax.rem(r + parts // 2, parts)
        return chip * 2 + c, j * PIECE

    def piece(d, r, c):
        slot, at = place(d, r, c)
        return gathered.at[slot, pl.ds(pl.multiple_of(at, PIECE), PIECE)]

    def ring_copy(d, ref, t):
        return pltpu.make_async_remote_copy(
            src_ref=ref,
            dst_ref=ref,
            send_sem=ring_send.at[d, t],
            recv_sem=ring_recv.at[d, t],
            device_id={"row": nexts[d]},
            device_id_type=MESH,
        )

    def sib_copy(ref, d, r):
        return pltpu.make_async_remote_copy(
            src_ref=ref,
            dst_ref=ref,
            send_sem=sib_send.at[d, r],
            recv_sem=sib_recv.at[d, r],
            device_id={"row": sib},
            device_id_type=MESH,
        )

    def own_piece(d, t):
        j = t if d == 0 else (t + parts // 2) % parts
        return gathered.at[me, pl.ds(j * PIECE, PIECE)]

    get_lat.wait()
    for t in range(parts):
        for d in range(2):
            ring_copy(d, own_piece(d, t), t).start()
    own_to_sib = sib_copy(gathered.at[me], 0, steps)
    own_to_sib.start()

    def stats_copy(buf, which, k):
        return pltpu.make_async_remote_copy(
            src_ref=buf.at[0],
            dst_ref=buf.at[k],
            send_sem=st_send.at[which],
            recv_sem=st_recv.at[which],
            device_id={"row": lax.rem(me + k, n)},
            device_id_type=MESH,
        )

    def stats_all(buf, which):
        return pltpu.make_async_remote_copy(
            src_ref=buf.at[pl.ds(1, n - 1)],
            dst_ref=buf.at[pl.ds(1, n - 1)],
            send_sem=st_send.at[which],
            recv_sem=st_recv.at[which],
            device_id={"row": sib},
            device_id_type=MESH,
        )

    x = gathered[me].astype(F32)
    mean, second = channel_stats(x)
    st1[0, 0:1] = mean
    st1[0, 1:2] = second
    for k in range(1, n):
        stats_copy(st1, 0, k).start()

    gets[2].wait()
    gets[3].wait()
    wv_v[...] = dot(wv_v[...], wo_v[...]).astype(BF16)

    def comm(r):
        for d in range(2):
            ref = piece(d, r, core)
            ring_copy(d, ref, r).wait_recv()

            @pl.when(r < steps - parts)
            def _():
                ring_copy(d, ref, r + parts).start()

            sib_copy(ref, d, r).start()

    comm(0)
    comm(1)
    stats_all(st1, 0).wait_recv()
    get_vec.wait()
    a1, b1 = affine(st1[:, 0], st1[:, 1], float(count), vec[0:1], vec[1:2])
    gets[0].wait()
    gets[1].wait()
    normed = (x * a1 + b1).astype(BF16)
    queries = dot(normed, wq_v[...]).astype(BF16)
    q_v[...] = (dot_t(queries, wk_v[...]) * (a1 * (LOG2E / C**0.5))).astype(BF16)

    m_v[...] = jnp.full_like(m_v, -1e30)
    l_v[...] = jnp.zeros_like(l_v)
    acc_v[...] = jnp.zeros_like(acc_v)

    def attend(keys):
        s = dot_t(q_v[...], keys)
        old = m_v[...]
        new = jnp.maximum(old, jnp.max(s, axis=1, keepdims=True))
        scale = jnp.exp2(old - new)
        p = jnp.exp2(s - new[:, :1]).astype(BF16)
        wide = p.astype(F32)
        l_v[...] = l_v[...] * scale + sum(
            wide[:, i : i + 128] for i in range(0, wide.shape[1], 128)
        )
        acc_v[...] = acc_v[...] * scale[:, :1] + dot(p, keys)
        m_v[...] = new

    def attend_shard(slot):
        for i in range(0, count, 2 * PIECE):
            attend(gathered[slot, pl.ds(i, 2 * PIECE)])

    def attend_pieces(r, c):
        attend(jnp.concatenate([piece(0, r, c)[...], piece(1, r, c)[...]], axis=0))

    def compute(r):
        attend_pieces(r, core)
        for d in range(2):
            sib_copy(piece(d, r, 1 - core), d, r).wait_recv()
        attend_pieces(r, 1 - core)

    attend_shard(me)
    sib_copy(gathered.at[sib], 0, steps).wait_recv()
    attend_shard(sib)
    compute(0)

    def step(r, carry):
        compute(r - 1)
        comm(r)
        return carry

    lax.fori_loop(2, steps, step, 0)
    compute(steps - 1)

    total = jnp.sum(l_v[...], axis=1, keepdims=True)
    attended = (acc_v[...] / total * a1 + b1).astype(BF16)
    hidden = (gathered[me].astype(F32) + dot(attended, wv_v[...])).astype(BF16)
    hid_v[...] = hidden

    def halo_copy(i):
        rows = pl.ds(count - W, W) if i == 0 else pl.ds(0, W)
        peer = lax.rem(me + 1, n) if i == 0 else lax.rem(me + n - 1, n)
        return pltpu.make_async_remote_copy(
            src_ref=hid_v.at[rows],
            dst_ref=halo_v.at[i],
            send_sem=halo_send.at[i],
            recv_sem=halo_recv.at[i],
            device_id={"row": peer},
            device_id_type=MESH,
        )

    h = hidden.astype(F32)
    mean, second = channel_stats(h)
    st2[0, 0:1] = mean
    st2[0, 1:2] = second
    for k in range(1, n):
        stats_copy(st2, 1, k).start()
    for i in range(2):
        halo_copy(i).start()
    gets[4].wait()
    stats_all(st2, 1).wait_recv()
    a2, b2 = affine(st2[:, 0], st2[:, 1], float(count), vec[2:3], vec[3:4])
    for i in range(2):
        halo_copy(i).wait_recv()

    col = lax.broadcasted_iota(jnp.int32, (W, C), 0)
    image_rows = count // W
    for b in range(image_rows + 2):
        if b == 0:
            f = halo_v[0]
        elif b == image_rows + 1:
            f = halo_v[1]
        else:
            f = hid_v[pl.ds((b - 1) * W, W)]
        v = f.astype(F32) * a2 + b2
        v = v / (1.0 + jnp.exp(-v))
        if b == 0:
            v = jnp.where(me > 0, v, 0.0)
        elif b == image_rows + 1:
            v = jnp.where(me < n - 1, v, 0.0)
        rows = pl.ds(b * W, W)
        act_v[rows, pl.ds(0, C)] = jnp.where(col == 0, 0.0, pltpu.roll(v, 1, 0)).astype(BF16)
        act_v[rows, pl.ds(C, C)] = v.astype(BF16)
        act_v[rows, pl.ds(2 * C, C)] = jnp.where(col == W - 1, 0.0, pltpu.roll(v, W - 1, 0)).astype(
            BF16
        )

    conv = dot(act_v[pl.ds(0, count)], wc_v[0])
    conv = conv + dot(act_v[pl.ds(W, count)], wc_v[1])
    conv = conv + dot(act_v[pl.ds(2 * W, count)], wc_v[2])
    out[...] = (hid_v[...].astype(F32) + (conv + vec[4:5])).astype(BF16)

    for t in range(parts):
        for d in range(2):
            ring_copy(d, own_piece(d, t), t).wait_send()

    def drain(r, carry):
        for d in range(2):
            ref = piece(d, r, core)

            @pl.when(r < steps - parts)
            def _():
                ring_copy(d, ref, r + parts).wait_send()

            sib_copy(ref, d, r).wait_send()
        return carry

    lax.fori_loop(0, steps, drain, 0)
    own_to_sib.wait_send()
    stats_all(st1, 0).wait_send()
    stats_all(st2, 1).wait_send()
    for i in range(2):
        halo_copy(i).wait_send()


def local(n, latent, g1, s1, w_query, w_key, w_value, w_out, g2, s2, w_conv, bias):
    rows = latent.shape[0]
    count = rows * W
    parts = count // PIECE
    steps = (n // 4 - 1) * parts + parts // 2
    vecs = jnp.stack([g1, s1, g2, s2, bias, bias, bias, bias])
    dma = pltpu.SemaphoreType.DMA
    vm = pltpu.VMEM
    result = pl.pallas_call(
        functools.partial(kernel, n),
        name="block",
        out_shape=jax.ShapeDtypeStruct((count, C), BF16),
        in_specs=[pl.BlockSpec(memory_space=pl.ANY)] * 7,
        out_specs=pl.BlockSpec(memory_space=pltpu.VMEM),
        scratch_shapes=[
            vm((n, count, C), BF16),
            vm((8, C), F32),
            vm((C, C), BF16),
            vm((C, C), BF16),
            vm((C, C), BF16),
            vm((C, C), BF16),
            vm((3, 3 * C, C), BF16),
            vm((count, C), BF16),
            vm((count, 128), F32),
            vm((count, 128), F32),
            vm((count, C), F32),
            vm((count, C), BF16),
            vm((2, W, C), BF16),
            vm((count + 2 * W, 3 * C), BF16),
            vm((n, 2, C), F32),
            vm((n, 2, C), F32),
            dma((7,)),
            dma((2, steps)),
            dma((2, steps)),
            dma((2, steps + 1)),
            dma((2, steps + 1)),
            dma((2,)),
            dma((2,)),
            dma((2,)),
            dma((2,)),
        ],
        compiler_params=pltpu.CompilerParams(
            collective_id=0, has_side_effects=True, vmem_limit_bytes=60 * 1024 * 1024
        ),
    )(
        latent.reshape(count, C),
        vecs,
        w_query,
        w_key,
        w_value,
        w_out,
        w_conv.reshape(3, 3 * C, C),
    )
    return result.reshape(rows, W, C)


def solution(mesh):
    n = mesh.shape["row"]
    in_specs = (P(("img", "row"), None, None), P(), P(), P(), P(), P(), P(), P(), P(), P(), P())
    return jax.shard_map(
        functools.partial(local, n),
        mesh=mesh,
        in_specs=in_specs,
        out_specs=P(("img", "row"), None, None),
        check_vma=False,
    )
```

```python
import functools

import jax
import jax.numpy as jnp
from jax import lax
from jax.experimental import pallas as pl
from jax.experimental.pallas import tpu as pltpu
from jax.sharding import PartitionSpec as P

MESH = pl.DeviceIdType.MESH
C = 512
GROUP = 16
W = 128
EPS = 1e-06
PIECE = 128
LOG2E = 1.4426950408889634
F32 = jnp.float32
BF16 = jnp.bfloat16


def group_total(x):
    lane = lax.broadcasted_iota(jnp.int32, x.shape, 1)
    width = x.shape[1]
    for s in (1, 2, 4, 8):
        up = pltpu.roll(x, s, 1)
        down = pltpu.roll(x, width - s, 1)
        x = x + jnp.where((lane // s) % 2 == 1, up, down)
    return x


def channel_stats(x):
    mean = jnp.sum(x, axis=0, keepdims=True) * (1.0 / x.shape[0])
    off = x - mean
    return mean, jnp.sum(off * off, axis=0, keepdims=True)


def group_mean(mean):
    return group_total(jnp.broadcast_to(mean, (8, C)))[:1] * (1.0 / GROUP)


def affine(means, seconds, near, count, gain, shift):
    devices = means.shape[0]
    off = means - near
    first = jnp.sum(off, axis=0, keepdims=True)
    second = jnp.sum(seconds + count * (off * off), axis=0, keepdims=True)
    row = lax.broadcasted_iota(jnp.int32, (8, C), 0)
    both = group_total(jnp.where(row == 0, first, second))
    offset = both[0:1] * (1.0 / (devices * GROUP))
    spread = both[1:2] * (1.0 / (devices * GROUP * count)) - offset * offset
    a = lax.rsqrt(jnp.maximum(spread, 0.0) + EPS) * gain
    return a, shift - (near + offset) * a


def dot(x, y):
    return jnp.dot(x, y, preferred_element_type=F32)


def dot_t(x, y):
    return lax.dot_general(x, y, (((1,), (1,)), ((), ())), preferred_element_type=F32)


def kernel(
    n,
    lat,
    g1,
    s1,
    g2,
    s2,
    bias,
    wq,
    wk,
    wv,
    wo,
    wc,
    out,
    gathered,
    vec,
    wq_v,
    wk_v,
    wv_v,
    wo_v,
    wc_v,
    q_v,
    m_v,
    l_v,
    acc_v,
    hid_v,
    halo_v,
    act_v,
    st1,
    st2,
    local_sem,
    ring_send,
    ring_recv,
    sib_send,
    sib_recv,
    heard,
    st_send,
    st_recv,
    halo_send,
    halo_recv,
):
    me = lax.axis_index("row")
    chips = n // 2
    z, core = me // 2, me % 2
    sib = me + 1 - 2 * core
    count = lat.shape[0]
    parts = count // PIECE
    half = chips // 2
    steps = (half - 1) * parts + parts // 2
    nexts = (
        lax.rem(z + 1, chips) * 2 + core,
        lax.rem(z + chips - 1, chips) * 2 + core,
    )
    near = (sib,) + nexts + tuple(peer + 1 - 2 * core for peer in nexts)

    get_lat = pltpu.make_async_copy(lat, gathered.at[me], local_sem.at[0])
    get_lat.start()
    gets = []
    get_vecs = []
    for i, a in enumerate((g1, s1, g2, s2, bias)):
        get_vecs.append(pltpu.make_async_copy(a, vec.at[i], local_sem.at[7 + i]))
        get_vecs[-1].start()
    for i, (a, b) in enumerate(((wq, wq_v), (wk, wk_v), (wv, wv_v), (wo, wo_v), (wc, wc_v))):
        gets.append(pltpu.make_async_copy(a, b, local_sem.at[2 + i]))
        gets[-1].start()

    def greet(semaphore):
        for peer in near:
            pl.semaphore_signal(semaphore, inc=1, device_id={"row": peer}, device_id_type=MESH)

    barrier = pltpu.get_barrier_semaphore()
    greet(barrier)
    pl.semaphore_wait(barrier, len(near))

    def place(d, r, c):
        hop = 1 + r // parts
        chip = lax.rem(z + chips - hop, chips) if d == 0 else lax.rem(z + hop, chips)
        j = lax.rem(r, parts) if d == 0 else lax.rem(r + parts // 2, parts)
        return chip * 2 + c, j * PIECE

    def piece(d, r, c):
        slot, at = place(d, r, c)
        return gathered.at[slot, pl.ds(pl.multiple_of(at, PIECE), PIECE)]

    def ring_copy(d, ref, t):
        return pltpu.make_async_remote_copy(
            src_ref=ref,
            dst_ref=ref,
            send_sem=ring_send.at[d, t],
            recv_sem=ring_recv.at[d, t],
            device_id={"row": nexts[d]},
            device_id_type=MESH,
        )

    def sib_copy(ref, d, r):
        return pltpu.make_async_remote_copy(
            src_ref=ref,
            dst_ref=ref,
            send_sem=sib_send.at[d, r],
            recv_sem=sib_recv.at[d, r],
            device_id={"row": sib},
            device_id_type=MESH,
        )

    def own_piece(d, t):
        j = t if d == 0 else (t + parts // 2) % parts
        return gathered.at[me, pl.ds(j * PIECE, PIECE)]

    get_lat.wait()
    for t in range(parts):
        for d in range(2):
            ring_copy(d, own_piece(d, t), t).start()
    own_to_sib = sib_copy(gathered.at[me], 0, steps)
    own_to_sib.start()
    greet(heard.at[0])

    def stats_copy(buf, which, k):
        return pltpu.make_async_remote_copy(
            src_ref=buf.at[0],
            dst_ref=buf.at[k],
            send_sem=st_send.at[which],
            recv_sem=st_recv.at[which],
            device_id={"row": lax.rem(me + k, n)},
            device_id_type=MESH,
        )

    def stats_all(buf, which):
        return pltpu.make_async_remote_copy(
            src_ref=buf.at[pl.ds(1, n - 1)],
            dst_ref=buf.at[pl.ds(1, n - 1)],
            send_sem=st_send.at[which],
            recv_sem=st_recv.at[which],
            device_id={"row": sib},
            device_id_type=MESH,
        )

    mean, second = channel_stats(gathered[me].astype(F32))
    st1[0, 0:1] = mean
    st1[0, 1:2] = second
    rounds = chips // 2 - 1
    for k in range(rounds):
        pl.semaphore_wait(heard.at[k], len(near))
        if k + 1 < rounds:
            greet(heard.at[k + 1])
    for k in range(1, n):
        stats_copy(st1, 0, k).start()
    near1 = group_mean(mean)

    gets[2].wait()
    gets[3].wait()
    wv_v[...] = dot(wv_v[...], wo_v[...]).astype(BF16)

    def comm(r):
        for d in range(2):
            ref = piece(d, r, core)
            ring_copy(d, ref, r).wait_recv()

            @pl.when(r < steps - parts)
            def _():
                ring_copy(d, ref, r + parts).start()

            sib_copy(ref, d, r).start()

    comm(0)
    comm(1)
    stats_all(st1, 0).wait_recv()
    for g in get_vecs:
        g.wait()
    a1, b1 = affine(st1[:, 0], st1[:, 1], near1, float(count), vec[0], vec[1])
    gets[0].wait()
    gets[1].wait()
    normed = (gathered[me].astype(F32) * a1 + b1).astype(BF16)
    queries = dot(normed, wq_v[...]).astype(BF16)
    q_v[...] = (dot_t(queries, wk_v[...]) * (a1 * (LOG2E / C**0.5))).astype(BF16)

    m_v[...] = jnp.full_like(m_v, -1e30)
    l_v[...] = jnp.zeros_like(l_v)
    acc_v[...] = jnp.zeros_like(acc_v)

    def wide(x, width):
        return jnp.concatenate([x] * (width // 128), axis=1)

    def attend(keys):
        width = keys.shape[0]
        halves = [pl.ds(i * (count // 2), count // 2) for i in range(2)]
        scores = [dot_t(q_v[h], keys) for h in halves]
        for h, s in zip(halves, scores):
            old = m_v[h]
            new = jnp.maximum(old, jnp.max(s, axis=1, keepdims=True))
            scale = jnp.exp2(old - new)
            p = jnp.exp2(s - wide(new, width)).astype(BF16)
            back = p.astype(F32)
            l_v[h] = l_v[h] * scale + sum(back[:, i : i + 128] for i in range(0, width, 128))
            acc_v[h] = acc_v[h] * wide(scale, C) + dot(p, keys)
            m_v[h] = new

    def pieces(r, c):
        return [piece(0, r, c)[...], piece(1, r, c)[...]]

    def compute(r):
        for d in range(2):
            sib_copy(piece(d, r, 1 - core), d, r).wait_recv()
        attend(jnp.concatenate(pieces(r, core) + pieces(r, 1 - core), axis=0))

    attend(gathered[me])
    sib_copy(gathered.at[sib], 0, steps).wait_recv()
    attend(gathered[sib])
    compute(0)

    def step(r, carry):
        compute(r - 1)
        comm(r)
        return carry

    lax.fori_loop(2, steps, step, 0)
    attend(jnp.concatenate(pieces(steps - 1, core), axis=0))
    for d in range(2):
        sib_copy(piece(d, steps - 1, 1 - core), d, steps - 1).wait_recv()
    attend(jnp.concatenate(pieces(steps - 1, 1 - core), axis=0))

    total = jnp.sum(l_v[...], axis=1, keepdims=True)
    attended = (acc_v[...] * (1.0 / total) * a1 + b1).astype(BF16)
    hidden = (gathered[me].astype(F32) + dot(attended, wv_v[...])).astype(BF16)
    hid_v[...] = hidden

    def halo_copy(i):
        rows = pl.ds(count - W, W) if i == 0 else pl.ds(0, W)
        peer = lax.rem(me + 1, n) if i == 0 else lax.rem(me + n - 1, n)
        return pltpu.make_async_remote_copy(
            src_ref=hid_v.at[rows],
            dst_ref=halo_v.at[i],
            send_sem=halo_send.at[i],
            recv_sem=halo_recv.at[i],
            device_id={"row": peer},
            device_id_type=MESH,
        )

    h = hidden.astype(F32)
    mean, second = channel_stats(h)
    st2[0, 0:1] = mean
    st2[0, 1:2] = second
    for k in range(1, n):
        stats_copy(st2, 1, k).start()
    for i in range(2):
        halo_copy(i).start()
    near2 = group_mean(mean)
    gets[4].wait()
    stats_all(st2, 1).wait_recv()
    a2, b2 = affine(st2[:, 0], st2[:, 1], near2, float(count), vec[2], vec[3])
    for i in range(2):
        halo_copy(i).wait_recv()

    col = lax.broadcasted_iota(jnp.int32, (W, C), 0)
    image_rows = count // W
    for b in range(image_rows + 2):
        if b == 0:
            f = halo_v[0]
        elif b == image_rows + 1:
            f = halo_v[1]
        else:
            f = hid_v[pl.ds((b - 1) * W, W)]
        v = f.astype(F32) * a2 + b2
        v = v / (1.0 + jnp.exp(-v))
        if b == 0:
            v = jnp.where(me > 0, v, 0.0)
        elif b == image_rows + 1:
            v = jnp.where(me < n - 1, v, 0.0)
        rows = pl.ds(b * W, W)
        act_v[rows, pl.ds(0, C)] = jnp.where(col == 0, 0.0, pltpu.roll(v, 1, 0)).astype(BF16)
        act_v[rows, pl.ds(C, C)] = v.astype(BF16)
        act_v[rows, pl.ds(2 * C, C)] = jnp.where(col == W - 1, 0.0, pltpu.roll(v, W - 1, 0)).astype(
            BF16
        )

    conv = dot(act_v[pl.ds(0, count)], wc_v[0])
    conv = conv + dot(act_v[pl.ds(W, count)], wc_v[1])
    conv = conv + dot(act_v[pl.ds(2 * W, count)], wc_v[2])
    out[...] = (hid_v[...].astype(F32) + (conv + vec[4])).astype(BF16)

    for t in range(parts):
        for d in range(2):
            ring_copy(d, own_piece(d, t), t).wait_send()

    def drain(r, carry):
        for d in range(2):
            ref = piece(d, r, core)

            @pl.when(r < steps - parts)
            def _():
                ring_copy(d, ref, r + parts).wait_send()

            sib_copy(ref, d, r).wait_send()
        return carry

    lax.fori_loop(0, steps, drain, 0)
    own_to_sib.wait_send()
    stats_all(st1, 0).wait_send()
    stats_all(st2, 1).wait_send()
    for i in range(2):
        halo_copy(i).wait_send()


def local(n, latent, g1, s1, w_query, w_key, w_value, w_out, g2, s2, w_conv, bias):
    rows = latent.shape[0]
    count = rows * W
    parts = count // PIECE
    steps = (n // 4 - 1) * parts + parts // 2
    dma = pltpu.SemaphoreType.DMA
    vm = pltpu.VMEM
    result = pl.pallas_call(
        functools.partial(kernel, n),
        name="block",
        out_shape=jax.ShapeDtypeStruct((count, C), BF16),
        in_specs=[pl.BlockSpec(memory_space=pl.ANY)] * 11,
        out_specs=pl.BlockSpec(memory_space=pltpu.VMEM),
        scratch_shapes=[
            vm((n, count, C), BF16),
            vm((5, 1, C), F32),
            vm((C, C), BF16),
            vm((C, C), BF16),
            vm((C, C), BF16),
            vm((C, C), BF16),
            vm((3, 3 * C, C), BF16),
            vm((count, C), BF16),
            vm((count, 128), F32),
            vm((count, 128), F32),
            vm((count, C), F32),
            vm((count, C), BF16),
            vm((2, W, C), BF16),
            vm((count + 2 * W, 3 * C), BF16),
            vm((n, 2, C), F32),
            vm((n, 2, C), F32),
            dma((12,)),
            dma((2, steps)),
            dma((2, steps)),
            dma((2, steps + 1)),
            dma((2, steps + 1)),
            pltpu.SemaphoreType.REGULAR((n // 4 - 1,)),
            dma((2,)),
            dma((2,)),
            dma((2,)),
            dma((2,)),
        ],
        compiler_params=pltpu.CompilerParams(
            collective_id=0, has_side_effects=True, vmem_limit_bytes=60 * 1024 * 1024
        ),
    )(
        latent.reshape(count, C),
        *(v.reshape(1, C) for v in (g1, s1, g2, s2, bias)),
        w_query,
        w_key,
        w_value,
        w_out,
        w_conv.reshape(3, 3 * C, C),
    )
    return result.reshape(rows, W, C)


def solution(mesh):
    n = mesh.shape["row"]
    in_specs = (P(("img", "row"), None, None), P(), P(), P(), P(), P(), P(), P(), P(), P(), P())
    return jax.shard_map(
        functools.partial(local, n),
        mesh=mesh,
        in_specs=in_specs,
        out_specs=P(("img", "row"), None, None),
        check_vma=False,
    )
```

```python
import functools

import jax
import jax.numpy as jnp
from jax import lax
from jax.experimental import pallas as pl
from jax.experimental.pallas import tpu as pltpu
from jax.sharding import PartitionSpec as P

MESH = pl.DeviceIdType.MESH
C = 512
GROUP = 16
W = 128
EPS = 1e-06
PIECE = 128
LOG2E = 1.4426950408889634
F32 = jnp.float32
BF16 = jnp.bfloat16


def group_total(x):
    lane = lax.broadcasted_iota(jnp.int32, x.shape, 1)
    width = x.shape[1]
    for s in (1, 2, 4, 8):
        up = pltpu.roll(x, s, 1)
        down = pltpu.roll(x, width - s, 1)
        x = x + jnp.where((lane // s) % 2 == 1, up, down)
    return x


def channel_stats(x):
    mean = jnp.sum(x, axis=0, keepdims=True) * (1.0 / x.shape[0])
    off = x - mean
    return mean, jnp.sum(off * off, axis=0, keepdims=True)


def tiles(row):
    at = lax.broadcasted_iota(jnp.int32, (8, 128), 0) % (C // 128)
    out = jnp.broadcast_to(row[:, :128], (8, 128))
    for k in range(1, C // 128):
        out = jnp.where(at == k, row[:, 128 * k : 128 * (k + 1)], out)
    return out


def line(x):
    lane = lax.broadcasted_iota(jnp.int32, (8, 128), 1) % GROUP
    at = lax.broadcasted_iota(jnp.int32, (8, 128), 0)
    return jnp.sum(jnp.where(lane == at, x, 0.0), axis=0, keepdims=True)


def group_stats(mean, second, count):
    mean, second = tiles(mean), tiles(second)
    centre = group_total(mean) * (1.0 / GROUP)
    off = mean - centre
    return line(centre), line(group_total(second + count * (off * off)))


def affine(means, seconds, count, gain, shift):
    devices = means.shape[0]
    centre = jnp.sum(means, axis=0, keepdims=True) * (1.0 / devices)
    off = means - centre
    size = count * GROUP
    second = jnp.sum(seconds + size * (off * off), axis=0, keepdims=True)
    scale = lax.rsqrt(second * (1.0 / (devices * size)) + EPS)
    at = lax.broadcasted_iota(jnp.int32, (8, 128), 0)
    lane = lax.broadcasted_iota(jnp.int32, (8, 128), 1) % GROUP
    both = jnp.where(at < C // 128, centre, scale)
    both = group_total(jnp.where(lane == at % (C // 128), both, 0.0))
    centre, scale = (
        jnp.concatenate([both[k : k + 1] for k in range(first, first + C // 128)], axis=1)
        for first in (0, C // 128)
    )
    a = scale * gain
    return a, shift - centre * a


def dot(x, y):
    return jnp.dot(x, y, preferred_element_type=F32)


def dot_t(x, y):
    return lax.dot_general(x, y, (((1,), (1,)), ((), ())), preferred_element_type=F32)


def kernel(
    n,
    lat,
    g1,
    s1,
    g2,
    s2,
    bias,
    wq,
    wk,
    wv,
    wo,
    wc,
    out,
    gathered,
    vec,
    wq_v,
    wk_v,
    wv_v,
    wo_v,
    wc_v,
    q_v,
    m_v,
    l_v,
    acc_v,
    hid_v,
    halo_v,
    act_v,
    st1,
    st2,
    local_sem,
    ring_send,
    ring_recv,
    sib_send,
    sib_recv,
    heard,
    st_send,
    st_recv,
    halo_send,
    halo_recv,
):
    me = lax.axis_index("row")
    chips = n // 2
    z, core = me // 2, me % 2
    sib = me + 1 - 2 * core
    count = lat.shape[0]
    parts = count // PIECE
    half = chips // 2
    steps = (half - 1) * parts + parts // 2
    nexts = (
        lax.rem(z + 1, chips) * 2 + core,
        lax.rem(z + chips - 1, chips) * 2 + core,
    )
    near = (sib,) + nexts + tuple(peer + 1 - 2 * core for peer in nexts)

    get_lat = pltpu.make_async_copy(lat, gathered.at[me], local_sem.at[0])
    get_lat.start()
    gets = []
    get_vecs = []
    for i, a in enumerate((g1, s1, g2, s2, bias)):
        get_vecs.append(pltpu.make_async_copy(a, vec.at[i], local_sem.at[7 + i]))
        get_vecs[-1].start()
    for i, (a, b) in enumerate(((wq, wq_v), (wk, wk_v), (wv, wv_v), (wo, wo_v), (wc, wc_v))):
        gets.append(pltpu.make_async_copy(a, b, local_sem.at[2 + i]))
        gets[-1].start()

    def greet(semaphore):
        for peer in near:
            pl.semaphore_signal(semaphore, inc=1, device_id={"row": peer}, device_id_type=MESH)

    barrier = pltpu.get_barrier_semaphore()
    greet(barrier)
    pl.semaphore_wait(barrier, len(near))

    def place(d, r, c):
        hop = 1 + r // parts
        chip = lax.rem(z + chips - hop, chips) if d == 0 else lax.rem(z + hop, chips)
        j = lax.rem(r, parts) if d == 0 else lax.rem(r + parts // 2, parts)
        return chip * 2 + c, j * PIECE

    def piece(d, r, c):
        slot, at = place(d, r, c)
        return gathered.at[slot, pl.ds(pl.multiple_of(at, PIECE), PIECE)]

    def ring_copy(d, ref, t):
        return pltpu.make_async_remote_copy(
            src_ref=ref,
            dst_ref=ref,
            send_sem=ring_send.at[d, t],
            recv_sem=ring_recv.at[d, t],
            device_id={"row": nexts[d]},
            device_id_type=MESH,
        )

    def sib_copy(ref, d, r):
        return pltpu.make_async_remote_copy(
            src_ref=ref,
            dst_ref=ref,
            send_sem=sib_send.at[d, r],
            recv_sem=sib_recv.at[d, r],
            device_id={"row": sib},
            device_id_type=MESH,
        )

    def own_piece(d, t):
        j = t if d == 0 else (t + parts // 2) % parts
        return gathered.at[me, pl.ds(j * PIECE, PIECE)]

    get_lat.wait()
    for t in range(parts):
        for d in range(2):
            ring_copy(d, own_piece(d, t), t).start()
    own_to_sib = sib_copy(gathered.at[me], 0, steps)
    own_to_sib.start()
    greet(heard.at[0])

    def stats_copy(buf, which, k):
        return pltpu.make_async_remote_copy(
            src_ref=buf.at[0],
            dst_ref=buf.at[k],
            send_sem=st_send.at[which],
            recv_sem=st_recv.at[which],
            device_id={"row": lax.rem(me + k, n)},
            device_id_type=MESH,
        )

    def stats_all(buf, which):
        return pltpu.make_async_remote_copy(
            src_ref=buf.at[pl.ds(1, n - 1)],
            dst_ref=buf.at[pl.ds(1, n - 1)],
            send_sem=st_send.at[which],
            recv_sem=st_recv.at[which],
            device_id={"row": sib},
            device_id_type=MESH,
        )

    mean, second = channel_stats(gathered[me].astype(F32))
    mean, second = group_stats(mean, second, float(count))
    st1[0, 0:1] = mean
    st1[0, 1:2] = second
    rounds = chips // 2 - 1
    for k in range(rounds):
        pl.semaphore_wait(heard.at[k], len(near))
        if k + 1 < rounds:
            greet(heard.at[k + 1])
    for k in range(1, n):
        stats_copy(st1, 0, k).start()

    gets[2].wait()
    gets[3].wait()
    wv_v[...] = dot(wv_v[...], wo_v[...]).astype(BF16)

    def comm(r):
        for d in range(2):
            ref = piece(d, r, core)
            ring_copy(d, ref, r).wait_recv()

            @pl.when(r < steps - parts)
            def _():
                ring_copy(d, ref, r + parts).start()

            sib_copy(ref, d, r).start()

    for r in range(parts):
        comm(r)
    stats_all(st1, 0).wait_recv()
    for g in get_vecs:
        g.wait()
    a1, b1 = affine(st1[:, 0], st1[:, 1], float(count), vec[0], vec[1])
    gets[0].wait()
    gets[1].wait()
    normed = (gathered[me].astype(F32) * a1 + b1).astype(BF16)
    queries = dot(normed, wq_v[...]).astype(BF16)
    q_v[...] = (dot_t(queries, wk_v[...]) * (a1 * (LOG2E / C**0.5))).astype(BF16)

    m_v[...] = jnp.full_like(m_v, -1e30)
    l_v[...] = jnp.zeros_like(l_v)
    acc_v[...] = jnp.zeros_like(acc_v)

    def wide(x, width):
        return jnp.concatenate([x] * (width // 128), axis=1)

    def attend(keys):
        width = keys.shape[0]
        halves = [pl.ds(i * (count // 2), count // 2) for i in range(2)]
        scores = [dot_t(q_v[h], keys) for h in halves]
        for h, s in zip(halves, scores):
            old = m_v[h]
            new = jnp.maximum(old, jnp.max(s, axis=1, keepdims=True))
            scale = jnp.exp2(old - new)
            p = jnp.exp2(s - wide(new, width)).astype(BF16)
            back = p.astype(F32)
            l_v[h] = l_v[h] * scale + sum(back[:, i : i + 128] for i in range(0, width, 128))
            acc_v[h] = acc_v[h] * wide(scale, C) + dot(p, keys)
            m_v[h] = new

    def pieces(r, c):
        return [piece(0, r, c)[...], piece(1, r, c)[...]]

    def compute(r):
        for d in range(2):
            sib_copy(piece(d, r, 1 - core), d, r).wait_recv()
        attend(jnp.concatenate(pieces(r, core) + pieces(r, 1 - core), axis=0))

    attend(gathered[me])
    sib_copy(gathered.at[sib], 0, steps).wait_recv()
    attend(gathered[sib])
    lax.fori_loop(0, parts - 1, lambda r, carry: (compute(r), carry)[1], 0)

    def step(r, carry):
        compute(r - 1)
        comm(r)
        return carry

    lax.fori_loop(parts, steps, step, 0)
    attend(jnp.concatenate(pieces(steps - 1, core), axis=0))
    for d in range(2):
        sib_copy(piece(d, steps - 1, 1 - core), d, steps - 1).wait_recv()
    attend(jnp.concatenate(pieces(steps - 1, 1 - core), axis=0))

    total = jnp.sum(l_v[...], axis=1, keepdims=True)
    attended = (acc_v[...] * (1.0 / total) * a1 + b1).astype(BF16)
    hidden = (gathered[me].astype(F32) + dot(attended, wv_v[...])).astype(BF16)
    hid_v[...] = hidden

    def halo_copy(i):
        rows = pl.ds(count - W, W) if i == 0 else pl.ds(0, W)
        peer = lax.rem(me + 1, n) if i == 0 else lax.rem(me + n - 1, n)
        return pltpu.make_async_remote_copy(
            src_ref=hid_v.at[rows],
            dst_ref=halo_v.at[i],
            send_sem=halo_send.at[i],
            recv_sem=halo_recv.at[i],
            device_id={"row": peer},
            device_id_type=MESH,
        )

    h = hidden.astype(F32)
    mean, second = channel_stats(h)
    mean, second = group_stats(mean, second, float(count))
    st2[0, 0:1] = mean
    st2[0, 1:2] = second
    for k in range(1, n):
        stats_copy(st2, 1, k).start()
    for i in range(2):
        halo_copy(i).start()
    gets[4].wait()
    stats_all(st2, 1).wait_recv()
    a2, b2 = affine(st2[:, 0], st2[:, 1], float(count), vec[2], vec[3])
    for i in range(2):
        halo_copy(i).wait_recv()

    col = lax.broadcasted_iota(jnp.int32, (W, C), 0)
    image_rows = count // W
    for b in range(image_rows + 2):
        if b == 0:
            f = halo_v[0]
        elif b == image_rows + 1:
            f = halo_v[1]
        else:
            f = hid_v[pl.ds((b - 1) * W, W)]
        v = f.astype(F32) * a2 + b2
        v = v / (1.0 + jnp.exp(-v))
        if b == 0:
            v = jnp.where(me > 0, v, 0.0)
        elif b == image_rows + 1:
            v = jnp.where(me < n - 1, v, 0.0)
        rows = pl.ds(b * W, W)
        act_v[rows, pl.ds(0, C)] = jnp.where(col == 0, 0.0, pltpu.roll(v, 1, 0)).astype(BF16)
        act_v[rows, pl.ds(C, C)] = v.astype(BF16)
        act_v[rows, pl.ds(2 * C, C)] = jnp.where(col == W - 1, 0.0, pltpu.roll(v, W - 1, 0)).astype(
            BF16
        )

    conv = dot(act_v[pl.ds(0, count)], wc_v[0])
    conv = conv + dot(act_v[pl.ds(W, count)], wc_v[1])
    conv = conv + dot(act_v[pl.ds(2 * W, count)], wc_v[2])
    out[...] = (hid_v[...].astype(F32) + (conv + vec[4])).astype(BF16)

    for t in range(parts):
        for d in range(2):
            ring_copy(d, own_piece(d, t), t).wait_send()

    def drain(r, carry):
        for d in range(2):
            ref = piece(d, r, core)

            @pl.when(r < steps - parts)
            def _():
                ring_copy(d, ref, r + parts).wait_send()

            sib_copy(ref, d, r).wait_send()
        return carry

    lax.fori_loop(0, steps, drain, 0)
    own_to_sib.wait_send()
    stats_all(st1, 0).wait_send()
    stats_all(st2, 1).wait_send()
    for i in range(2):
        halo_copy(i).wait_send()


def local(n, latent, g1, s1, w_query, w_key, w_value, w_out, g2, s2, w_conv, bias):
    rows = latent.shape[0]
    count = rows * W
    parts = count // PIECE
    steps = (n // 4 - 1) * parts + parts // 2
    dma = pltpu.SemaphoreType.DMA
    vm = pltpu.VMEM
    result = pl.pallas_call(
        functools.partial(kernel, n),
        name="block",
        out_shape=jax.ShapeDtypeStruct((count, C), BF16),
        in_specs=[pl.BlockSpec(memory_space=pl.ANY)] * 11,
        out_specs=pl.BlockSpec(memory_space=pltpu.VMEM),
        scratch_shapes=[
            vm((n, count, C), BF16),
            vm((5, 1, C), F32),
            vm((C, C), BF16),
            vm((C, C), BF16),
            vm((C, C), BF16),
            vm((C, C), BF16),
            vm((3, 3 * C, C), BF16),
            vm((count, C), BF16),
            vm((count, 128), F32),
            vm((count, 128), F32),
            vm((count, C), F32),
            vm((count, C), BF16),
            vm((2, W, C), BF16),
            vm((count + 2 * W, 3 * C), BF16),
            vm((n, 2, 128), F32),
            vm((n, 2, 128), F32),
            dma((12,)),
            dma((2, steps)),
            dma((2, steps)),
            dma((2, steps + 1)),
            dma((2, steps + 1)),
            pltpu.SemaphoreType.REGULAR((n // 4 - 1,)),
            dma((2,)),
            dma((2,)),
            dma((2,)),
            dma((2,)),
        ],
        compiler_params=pltpu.CompilerParams(
            collective_id=0, has_side_effects=True, vmem_limit_bytes=60 * 1024 * 1024
        ),
    )(
        latent.reshape(count, C),
        *(v.reshape(1, C) for v in (g1, s1, g2, s2, bias)),
        w_query,
        w_key,
        w_value,
        w_out,
        w_conv.reshape(3, 3 * C, C),
    )
    return result.reshape(rows, W, C)


def solution(mesh):
    n = mesh.shape["row"]
    in_specs = (P(("img", "row"), None, None), P(), P(), P(), P(), P(), P(), P(), P(), P(), P())
    return jax.shard_map(
        functools.partial(local, n),
        mesh=mesh,
        in_specs=in_specs,
        out_specs=P(("img", "row"), None, None),
        check_vma=False,
    )
```

```python
import functools

import jax
import jax.numpy as jnp
from jax import lax
from jax.experimental import pallas as pl
from jax.experimental.pallas import tpu as pltpu
from jax.sharding import PartitionSpec as P

MESH = pl.DeviceIdType.MESH
C = 512
GROUP = 16
W = 128
EPS = 1e-06
PIECE = 128
LOG2E = 1.4426950408889634
F32 = jnp.float32
BF16 = jnp.bfloat16


def group_total(x):
    lane = lax.broadcasted_iota(jnp.int32, x.shape, 1)
    width = x.shape[1]
    for s in (1, 2, 4, 8):
        up = pltpu.roll(x, s, 1)
        down = pltpu.roll(x, width - s, 1)
        x = x + jnp.where((lane // s) % 2 == 1, up, down)
    return x


def channel_stats(x):
    mean = jnp.sum(x, axis=0, keepdims=True) * (1.0 / x.shape[0])
    off = x - mean
    return mean, jnp.sum(off * off, axis=0, keepdims=True)


def tiles(row):
    at = lax.broadcasted_iota(jnp.int32, (8, 128), 0) % (C // 128)
    out = jnp.broadcast_to(row[:, :128], (8, 128))
    for k in range(1, C // 128):
        out = jnp.where(at == k, row[:, 128 * k : 128 * (k + 1)], out)
    return out


def line(x):
    lane = lax.broadcasted_iota(jnp.int32, (8, 128), 1) % GROUP
    at = lax.broadcasted_iota(jnp.int32, (8, 128), 0)
    return jnp.sum(jnp.where(lane == at, x, 0.0), axis=0, keepdims=True)


def group_stats(mean, second, count):
    mean, second = tiles(mean), tiles(second)
    centre = group_total(mean) * (1.0 / GROUP)
    off = mean - centre
    return line(centre), line(group_total(second + count * (off * off)))


def shifted_stats(x, near, count):
    off = x - near
    first = jnp.sum(off, axis=0, keepdims=True)
    second = jnp.sum(off * off, axis=0, keepdims=True)
    at = lax.broadcasted_iota(jnp.int32, (8, 128), 0)
    total = group_total(jnp.where(at < C // 128, tiles(first), tiles(second)))
    lane = lax.broadcasted_iota(jnp.int32, (8, 128), 1) % GROUP
    mine = jnp.where(lane == at % (C // 128), total, 0.0)
    first = jnp.sum(jnp.where(at < C // 128, mine, 0.0), axis=0, keepdims=True)
    second = jnp.sum(jnp.where(at < C // 128, 0.0, mine), axis=0, keepdims=True)
    offset = first * (1.0 / (GROUP * count))
    lanes = lax.broadcasted_iota(jnp.int32, (1, 128), 1) % GROUP
    base = near[:, :128]
    for k in range(1, C // 128):
        base = jnp.where(lanes == k, near[:, 128 * k : 128 * (k + 1)], base)
    return base + offset, jnp.maximum(second - first * offset, 0.0)


def affine(means, seconds, count, gain, shift):
    devices = means.shape[0]
    centre = jnp.sum(means, axis=0, keepdims=True) * (1.0 / devices)
    off = means - centre
    size = count * GROUP
    second = jnp.sum(seconds + size * (off * off), axis=0, keepdims=True)
    scale = lax.rsqrt(second * (1.0 / (devices * size)) + EPS)
    at = lax.broadcasted_iota(jnp.int32, (8, 128), 0)
    lane = lax.broadcasted_iota(jnp.int32, (8, 128), 1) % GROUP
    both = jnp.where(at < C // 128, centre, scale)
    both = group_total(jnp.where(lane == at % (C // 128), both, 0.0))
    centre, scale = (
        jnp.concatenate([both[k : k + 1] for k in range(first, first + C // 128)], axis=1)
        for first in (0, C // 128)
    )
    a = scale * gain
    return a, shift - centre * a, centre


def dot(x, y):
    return jnp.dot(x, y, preferred_element_type=F32)


def dot_t(x, y):
    return lax.dot_general(x, y, (((1,), (1,)), ((), ())), preferred_element_type=F32)


def kernel(
    n,
    lat,
    g1,
    s1,
    g2,
    s2,
    bias,
    wq,
    wk,
    wv,
    wo,
    wc,
    out,
    gathered,
    vec,
    wq_v,
    wk_v,
    wv_v,
    wo_v,
    wc_v,
    q_v,
    m_v,
    l_v,
    acc_v,
    hid_v,
    halo_v,
    act_v,
    st1,
    st2,
    local_sem,
    ring_send,
    ring_recv,
    sib_send,
    sib_recv,
    heard,
    st_send,
    st_recv,
    halo_send,
    halo_recv,
):
    me = lax.axis_index("row")
    chips = n // 2
    z, core = me // 2, me % 2
    sib = me + 1 - 2 * core
    count = lat.shape[0]
    parts = count // PIECE
    half = chips // 2
    steps = (half - 1) * parts + parts // 2
    nexts = (
        lax.rem(z + 1, chips) * 2 + core,
        lax.rem(z + chips - 1, chips) * 2 + core,
    )
    near = (sib,) + nexts + tuple(peer + 1 - 2 * core for peer in nexts)

    get_lat = pltpu.make_async_copy(lat, gathered.at[me], local_sem.at[0])
    get_lat.start()
    def greet(semaphore):
        for peer in near:
            pl.semaphore_signal(semaphore, inc=1, device_id={"row": peer}, device_id_type=MESH)

    barrier = pltpu.get_barrier_semaphore()
    greet(barrier)
    pl.semaphore_wait(barrier, len(near))

    def place(d, r, c):
        hop = 1 + r // parts
        chip = lax.rem(z + chips - hop, chips) if d == 0 else lax.rem(z + hop, chips)
        j = lax.rem(r, parts) if d == 0 else lax.rem(r + parts // 2, parts)
        return chip * 2 + c, j * PIECE

    def piece(d, r, c):
        slot, at = place(d, r, c)
        return gathered.at[slot, pl.ds(pl.multiple_of(at, PIECE), PIECE)]

    def ring_copy(d, ref, t):
        return pltpu.make_async_remote_copy(
            src_ref=ref,
            dst_ref=ref,
            send_sem=ring_send.at[d, t],
            recv_sem=ring_recv.at[d, t],
            device_id={"row": nexts[d]},
            device_id_type=MESH,
        )

    def sib_copy(ref, d, r):
        return pltpu.make_async_remote_copy(
            src_ref=ref,
            dst_ref=ref,
            send_sem=sib_send.at[d, r],
            recv_sem=sib_recv.at[d, r],
            device_id={"row": sib},
            device_id_type=MESH,
        )

    def own_piece(d, t):
        j = t if d == 0 else (t + parts // 2) % parts
        return gathered.at[me, pl.ds(j * PIECE, PIECE)]

    get_lat.wait()
    for t in range(parts):
        for d in range(2):
            ring_copy(d, own_piece(d, t), t).start()
    own_to_sib = sib_copy(gathered.at[me], 0, steps)
    own_to_sib.start()
    greet(heard.at[0])
    gets = []
    get_vecs = []
    for i, a in enumerate((g1, s1, g2, s2, bias)):
        get_vecs.append(pltpu.make_async_copy(a, vec.at[i], local_sem.at[7 + i]))
        get_vecs[-1].start()
    for i, (a, b) in enumerate(((wq, wq_v), (wk, wk_v), (wv, wv_v), (wo, wo_v))):
        gets.append(pltpu.make_async_copy(a, b, local_sem.at[2 + i]))
        gets[-1].start()
    get_taps = [
        pltpu.make_async_copy(wc.at[:, tap], wc_v.at[tap], local_sem.at[12 + tap]) for tap in range(3)
    ]
    for g in get_taps:
        g.start()


    farthest = sorted(range(1, n), key=lambda k: abs(k - n // 2))

    def stats_copy(buf, which, k):
        return pltpu.make_async_remote_copy(
            src_ref=buf.at[0],
            dst_ref=buf.at[k],
            send_sem=st_send.at[which],
            recv_sem=st_recv.at[which],
            device_id={"row": lax.rem(me + k, n)},
            device_id_type=MESH,
        )

    def stats_all(buf, which):
        return pltpu.make_async_remote_copy(
            src_ref=buf.at[pl.ds(1, n - 1)],
            dst_ref=buf.at[pl.ds(1, n - 1)],
            send_sem=st_send.at[which],
            recv_sem=st_recv.at[which],
            device_id={"row": sib},
            device_id_type=MESH,
        )

    mean, second = channel_stats(gathered[me].astype(F32))
    mean, second = group_stats(mean, second, float(count))
    st1[0, 0:1] = mean
    st1[0, 1:2] = second
    rounds = chips // 2 - 1
    for k in range(rounds):
        pl.semaphore_wait(heard.at[k], len(near))
        if k + 1 < rounds:
            greet(heard.at[k + 1])
    for k in farthest:
        stats_copy(st1, 0, k).start()

    gets[2].wait()
    gets[3].wait()
    wv_v[...] = dot(wv_v[...], wo_v[...]).astype(BF16)

    def comm(r):
        for d in range(2):
            ref = piece(d, r, core)
            ring_copy(d, ref, r).wait_recv()

            @pl.when(r < steps - parts)
            def _():
                ring_copy(d, ref, r + parts).start()

            sib_copy(ref, d, r).start()

    for r in range(parts):
        comm(r)
    stats_all(st1, 0).wait_recv()
    for g in get_vecs:
        g.wait()
    a1, b1, centre1 = affine(st1[:, 0], st1[:, 1], float(count), vec[0], vec[1])
    gets[0].wait()
    gets[1].wait()
    normed = (gathered[me].astype(F32) * a1 + b1).astype(BF16)
    queries = dot(normed, wq_v[...]).astype(BF16)
    q_v[...] = (dot_t(queries, wk_v[...]) * (a1 * (LOG2E / C**0.5))).astype(BF16)

    m_v[...] = jnp.full_like(m_v, -1e30)
    l_v[...] = jnp.zeros_like(l_v)
    acc_v[...] = jnp.zeros_like(acc_v)

    def wide(x, width):
        return jnp.concatenate([x] * (width // 128), axis=1)

    def attend(keys):
        width = keys.shape[0]
        halves = [pl.ds(i * (count // 2), count // 2) for i in range(2)]
        scores = [dot_t(q_v[h], keys) for h in halves]
        for h, s in zip(halves, scores):
            old = m_v[h]
            new = jnp.maximum(old, jnp.max(s, axis=1, keepdims=True))
            scale = jnp.exp2(old - new)
            p = jnp.exp2(s - wide(new, width)).astype(BF16)
            back = p.astype(F32)
            l_v[h] = l_v[h] * scale + sum(back[:, i : i + 128] for i in range(0, width, 128))
            acc_v[h] = acc_v[h] * wide(scale, C) + dot(p, keys)
            m_v[h] = new

    def pieces(r, c):
        return [piece(0, r, c)[...], piece(1, r, c)[...]]

    def compute(r):
        for d in range(2):
            sib_copy(piece(d, r, 1 - core), d, r).wait_recv()
        attend(jnp.concatenate(pieces(r, core) + pieces(r, 1 - core), axis=0))

    attend(gathered[me])
    sib_copy(gathered.at[sib], 0, steps).wait_recv()
    attend(gathered[sib])
    lax.fori_loop(0, parts - 1, lambda r, carry: (compute(r), carry)[1], 0)

    def step(r, carry):
        compute(r - 1)
        comm(r)
        return carry

    lax.fori_loop(parts, steps, step, 0)
    attend(jnp.concatenate(pieces(steps - 1, core), axis=0))
    for d in range(2):
        sib_copy(piece(d, steps - 1, 1 - core), d, steps - 1).wait_recv()
    attend(jnp.concatenate(pieces(steps - 1, 1 - core), axis=0))

    total = jnp.sum(l_v[...], axis=1, keepdims=True)
    attended = (acc_v[...] * (1.0 / total) * a1 + b1).astype(BF16)
    hidden = (gathered[me].astype(F32) + dot(attended, wv_v[...])).astype(BF16)
    hid_v[...] = hidden

    def halo_copy(i):
        rows = pl.ds(count - W, W) if i == 0 else pl.ds(0, W)
        peer = lax.rem(me + 1, n) if i == 0 else lax.rem(me + n - 1, n)
        return pltpu.make_async_remote_copy(
            src_ref=hid_v.at[rows],
            dst_ref=halo_v.at[i],
            send_sem=halo_send.at[i],
            recv_sem=halo_recv.at[i],
            device_id={"row": peer},
            device_id_type=MESH,
        )

    mean, second = shifted_stats(hidden.astype(F32), centre1, float(count))
    st2[0, 0:1] = mean
    st2[0, 1:2] = second
    for k in farthest:
        stats_copy(st2, 1, k).start()
    for i in range(2):
        halo_copy(i).start()
    for t in range(parts):
        for d in range(2):
            ring_copy(d, own_piece(d, t), t).wait_send()

    def drain(r, carry):
        for d in range(2):
            ref = piece(d, r, core)

            @pl.when(r < steps - parts)
            def _():
                ring_copy(d, ref, r + parts).wait_send()

            sib_copy(ref, d, r).wait_send()
        return carry

    lax.fori_loop(0, steps, drain, 0)
    for g in get_taps:
        g.wait()
    stats_all(st2, 1).wait_recv()
    a2, b2, _ = affine(st2[:, 0], st2[:, 1], float(count), vec[2], vec[3])
    for i in range(2):
        halo_copy(i).wait_recv()

    col = lax.broadcasted_iota(jnp.int32, (W, C), 0)
    image_rows = count // W

    def activate(b):
        if b == 0:
            f = halo_v[0]
        elif b == image_rows + 1:
            f = halo_v[1]
        else:
            f = hid_v[pl.ds((b - 1) * W, W)]
        v = f.astype(F32) * a2 + b2
        v = v / (1.0 + jnp.exp(-v))
        if b == 0:
            v = jnp.where(me > 0, v, 0.0)
        elif b == image_rows + 1:
            v = jnp.where(me < n - 1, v, 0.0)
        act_v[pl.ds(b * W, W)] = v.astype(BF16)

    part = image_rows // 2

    def convolve(h):
        around = jnp.concatenate(
            [act_v[pl.ds((h * part + i) * W, part * W)] for i in range(3)], axis=1
        )
        return {tap: dot(around, wc_v[tap].reshape(3 * C, C)) for tap in (0, 2, 1)}

    def finish(h, taps):
        for b in range(part):
            rows = slice(b * W, (b + 1) * W)
            left = jnp.where(col == 0, 0.0, pltpu.roll(taps[0][rows], 1, 0))
            right = jnp.where(col == W - 1, 0.0, pltpu.roll(taps[2][rows], W - 1, 0))
            conv = (left + right) + taps[1][rows]
            here = pl.ds((h * part + b) * W, W)
            out[here] = (hid_v[here].astype(F32) + (conv + vec[4])).astype(BF16)

    for b in range(part + 2):
        activate(b)
    first = convolve(0)
    for b in range(part + 2, image_rows + 2):
        activate(b)
    second = convolve(1)
    finish(0, first)
    finish(1, second)

    own_to_sib.wait_send()
    stats_all(st1, 0).wait_send()
    stats_all(st2, 1).wait_send()
    for i in range(2):
        halo_copy(i).wait_send()


def local(n, latent, g1, s1, w_query, w_key, w_value, w_out, g2, s2, w_conv, bias):
    rows = latent.shape[0]
    count = rows * W
    parts = count // PIECE
    steps = (n // 4 - 1) * parts + parts // 2
    dma = pltpu.SemaphoreType.DMA
    vm = pltpu.VMEM
    def stay(x):
        return pltpu.with_memory_space_constraint(x, pltpu.HBM)

    result = pl.pallas_call(
        functools.partial(kernel, n),
        name="block",
        out_shape=jax.ShapeDtypeStruct((count, C), BF16),
        in_specs=[pl.BlockSpec(memory_space=pl.ANY)] * 11,
        out_specs=pl.BlockSpec(memory_space=pltpu.VMEM),
        scratch_shapes=[
            vm((n, count, C), BF16),
            vm((5, 1, C), F32),
            vm((C, C), BF16),
            vm((C, C), BF16),
            vm((C, C), BF16),
            vm((C, C), BF16),
            vm((3, 3, C, C), BF16),
            vm((count, C), BF16),
            vm((count, 128), F32),
            vm((count, 128), F32),
            vm((count, C), F32),
            vm((count, C), BF16),
            vm((2, W, C), BF16),
            vm((count + 2 * W, C), BF16),
            vm((n, 2, 128), F32),
            vm((n, 2, 128), F32),
            dma((15,)),
            dma((2, steps)),
            dma((2, steps)),
            dma((2, steps + 1)),
            dma((2, steps + 1)),
            pltpu.SemaphoreType.REGULAR((n // 4 - 1,)),
            dma((2,)),
            dma((2,)),
            dma((2,)),
            dma((2,)),
        ],
        compiler_params=pltpu.CompilerParams(
            collective_id=0, has_side_effects=True, vmem_limit_bytes=40 * 1024 * 1024
        ),
    )(
        stay(latent.reshape(count, C)),
        *(stay(v.reshape(1, C)) for v in (g1, s1, g2, s2, bias)),
        stay(w_query),
        stay(w_key),
        stay(w_value),
        stay(w_out),
        stay(w_conv),
    )
    return result.reshape(rows, W, C)


def solution(mesh):
    n = mesh.shape["row"]
    in_specs = (P(("img", "row"), None, None), P(), P(), P(), P(), P(), P(), P(), P(), P(), P())
    return jax.shard_map(
        functools.partial(local, n),
        mesh=mesh,
        in_specs=in_specs,
        out_specs=P(("img", "row"), None, None),
        check_vma=False,
    )
```

```python
import functools

import jax
import jax.numpy as jnp
from jax import lax
from jax.experimental import pallas as pl
from jax.experimental.pallas import tpu as pltpu
from jax.sharding import PartitionSpec as P

MESH = pl.DeviceIdType.MESH
C = 512
GROUP = 16
W = 128
EPS = 1e-06
PIECE = 256
LAST = (128, 64, 64)
LOG2E = 1.4426950408889634
F32 = jnp.float32
BF16 = jnp.bfloat16


def group_total(x):
    lane = lax.broadcasted_iota(jnp.int32, x.shape, 1)
    width = x.shape[1]
    for s in (1, 2, 4, 8):
        up = pltpu.roll(x, s, 1)
        down = pltpu.roll(x, width - s, 1)
        x = x + jnp.where((lane // s) % 2 == 1, up, down)
    return x


def channel_stats(x):
    mean = jnp.sum(x, axis=0, keepdims=True) * (1.0 / x.shape[0])
    off = x - mean
    return mean, jnp.sum(off * off, axis=0, keepdims=True)


def tiles(row):
    at = lax.broadcasted_iota(jnp.int32, (8, 128), 0) % (C // 128)
    out = jnp.broadcast_to(row[:, :128], (8, 128))
    for k in range(1, C // 128):
        out = jnp.where(at == k, row[:, 128 * k : 128 * (k + 1)], out)
    return out


def line(x):
    lane = lax.broadcasted_iota(jnp.int32, (8, 128), 1) % GROUP
    at = lax.broadcasted_iota(jnp.int32, (8, 128), 0)
    return jnp.sum(jnp.where(lane == at, x, 0.0), axis=0, keepdims=True)


def group_stats(mean, second, count):
    mean, second = tiles(mean), tiles(second)
    centre = group_total(mean) * (1.0 / GROUP)
    off = mean - centre
    return line(centre), line(group_total(second + count * (off * off)))


def shifted_stats(x, near, count):
    off = x - near
    first = jnp.sum(off, axis=0, keepdims=True)
    second = jnp.sum(off * off, axis=0, keepdims=True)
    at = lax.broadcasted_iota(jnp.int32, (8, 128), 0)
    total = group_total(jnp.where(at < C // 128, tiles(first), tiles(second)))
    lane = lax.broadcasted_iota(jnp.int32, (8, 128), 1) % GROUP
    mine = jnp.where(lane == at % (C // 128), total, 0.0)
    first = jnp.sum(jnp.where(at < C // 128, mine, 0.0), axis=0, keepdims=True)
    second = jnp.sum(jnp.where(at < C // 128, 0.0, mine), axis=0, keepdims=True)
    offset = first * (1.0 / (GROUP * count))
    lanes = lax.broadcasted_iota(jnp.int32, (1, 128), 1) % GROUP
    base = near[:, :128]
    for k in range(1, C // 128):
        base = jnp.where(lanes == k, near[:, 128 * k : 128 * (k + 1)], base)
    return base + offset, jnp.maximum(second - first * offset, 0.0)


def affine(means, seconds, count, gain, shift):
    devices = means.shape[0]
    centre = jnp.sum(means, axis=0, keepdims=True) * (1.0 / devices)
    off = means - centre
    size = count * GROUP
    second = jnp.sum(seconds + size * (off * off), axis=0, keepdims=True)
    scale = lax.rsqrt(second * (1.0 / (devices * size)) + EPS)
    at = lax.broadcasted_iota(jnp.int32, (8, 128), 0)
    lane = lax.broadcasted_iota(jnp.int32, (8, 128), 1)
    both = jnp.where(at < C // 128, centre, scale)
    both = jnp.take_along_axis(both, lane // GROUP * GROUP + at % (C // 128), axis=1)
    centre, scale = (
        jnp.concatenate([both[k : k + 1] for k in range(first, first + C // 128)], axis=1)
        for first in (0, C // 128)
    )
    a = scale * gain
    return a, shift - centre * a, centre


def dot(x, y):
    return jnp.dot(x, y, preferred_element_type=F32)


def dot_t(x, y):
    return lax.dot_general(x, y, (((1,), (1,)), ((), ())), preferred_element_type=F32)


def kernel(
    n,
    lat,
    g1,
    s1,
    g2,
    s2,
    bias,
    wq,
    wk,
    wv,
    wo,
    wc,
    out,
    gathered,
    vec,
    wq_v,
    wk_v,
    wv_v,
    wo_v,
    wc_v,
    q_v,
    m_v,
    l_v,
    acc_v,
    hid_v,
    halo_v,
    act_v,
    st1,
    st2,
    local_sem,
    ring_send,
    ring_recv,
    sib_send,
    sib_recv,
    heard,
    st_send,
    st_recv,
    halo_send,
    halo_recv,
):
    me = lax.axis_index("row")
    chips = n // 2
    z, core = me // 2, me % 2
    sib = me + 1 - 2 * core
    count = lat.shape[0]
    parts = count // PIECE
    half = chips // 2
    steps = (half - 1) * parts
    ends = len(LAST)
    assert parts == 2 and sum(LAST) == PIECE
    nexts = (
        lax.rem(z + 1, chips) * 2 + core,
        lax.rem(z + chips - 1, chips) * 2 + core,
    )
    near = (sib,) + nexts + tuple(peer + 1 - 2 * core for peer in nexts)

    get_lat = pltpu.make_async_copy(lat, gathered.at[me], local_sem.at[0])
    get_lat.start()
    def greet(semaphore):
        for peer in near:
            pl.semaphore_signal(semaphore, inc=1, device_id={"row": peer}, device_id_type=MESH)

    barrier = pltpu.get_barrier_semaphore()
    greet(barrier)
    pl.semaphore_wait(barrier, len(near))

    def place(d, r, c):
        hop = 1 + r // parts
        chip = lax.rem(z + chips - hop, chips) if d == 0 else lax.rem(z + hop, chips)
        j = lax.rem(r, parts) if d == 0 else lax.rem(r + parts // 2, parts)
        return chip * 2 + c, j * PIECE

    def piece(d, r, c):
        slot, at = place(d, r, c)
        return gathered.at[slot, pl.ds(pl.multiple_of(at, PIECE), PIECE)]

    def last(d, k, c):
        at = (PIECE if d else 0) + sum(LAST[:k])
        return gathered.at[lax.rem(z + half, chips) * 2 + c, pl.ds(at, LAST[k])]

    def last_on(d, k):
        at = (PIECE if d else 0) + sum(LAST[:k])
        hop = half - 1
        chip = lax.rem(z + chips - hop, chips) if d == 0 else lax.rem(z + hop, chips)
        return gathered.at[chip * 2 + core, pl.ds(at, LAST[k])]

    def ring_copy(d, ref, t):
        return pltpu.make_async_remote_copy(
            src_ref=ref,
            dst_ref=ref,
            send_sem=ring_send.at[d, t],
            recv_sem=ring_recv.at[d, t],
            device_id={"row": nexts[d]},
            device_id_type=MESH,
        )

    def sib_copy(ref, d, r):
        return pltpu.make_async_remote_copy(
            src_ref=ref,
            dst_ref=ref,
            send_sem=sib_send.at[d, r],
            recv_sem=sib_recv.at[d, r],
            device_id={"row": sib},
            device_id_type=MESH,
        )

    def own_piece(d, t):
        j = t if d == 0 else (t + parts // 2) % parts
        return gathered.at[me, pl.ds(j * PIECE, PIECE)]

    get_lat.wait()
    for t in range(parts):
        for d in range(2):
            ring_copy(d, own_piece(d, t), t).start()
    own_to_sib = sib_copy(gathered.at[me], 0, steps + ends)
    own_to_sib.start()
    greet(heard.at[0])
    gets = []
    get_vecs = []
    for i, a in enumerate((g1, s1, g2, s2, bias)):
        get_vecs.append(pltpu.make_async_copy(a, vec.at[i], local_sem.at[7 + i]))
        get_vecs[-1].start()
    for i, (a, b) in enumerate(((wq, wq_v), (wk, wk_v), (wv, wv_v), (wo, wo_v))):
        gets.append(pltpu.make_async_copy(a, b, local_sem.at[2 + i]))
        gets[-1].start()
    get_taps = [
        pltpu.make_async_copy(wc.at[:, tap], wc_v.at[tap], local_sem.at[12 + tap]) for tap in range(3)
    ]
    for g in get_taps:
        g.start()


    farthest = sorted(range(1, n), key=lambda k: abs(k - n // 2))

    def stats_copy(buf, which, k):
        return pltpu.make_async_remote_copy(
            src_ref=buf.at[0],
            dst_ref=buf.at[k],
            send_sem=st_send.at[which],
            recv_sem=st_recv.at[which],
            device_id={"row": lax.rem(me + k, n)},
            device_id_type=MESH,
        )

    def alike_copy(k):
        return pltpu.make_async_remote_copy(
            src_ref=st1.at[0],
            dst_ref=st1.at[k // 2],
            send_sem=st_send.at[0],
            recv_sem=st_recv.at[0],
            device_id={"row": lax.rem(me + k, n)},
            device_id_type=MESH,
        )

    def alike_all():
        some = st1.at[pl.ds(1, chips - 1)]
        return pltpu.make_async_remote_copy(
            src_ref=some,
            dst_ref=some,
            send_sem=st_send.at[0],
            recv_sem=st_recv.at[0],
            device_id={"row": sib},
            device_id_type=MESH,
        )

    def alike_over():
        return pltpu.make_async_remote_copy(
            src_ref=st1.at[pl.ds(0, chips)],
            dst_ref=st1.at[pl.ds(chips, chips)],
            send_sem=st_send.at[2],
            recv_sem=st_recv.at[2],
            device_id={"row": sib},
            device_id_type=MESH,
        )

    def stats_all(buf, which):
        return pltpu.make_async_remote_copy(
            src_ref=buf.at[pl.ds(1, n - 1)],
            dst_ref=buf.at[pl.ds(1, n - 1)],
            send_sem=st_send.at[which],
            recv_sem=st_recv.at[which],
            device_id={"row": sib},
            device_id_type=MESH,
        )

    mean, second = channel_stats(gathered[me].astype(F32))
    mean, second = group_stats(mean, second, float(count))
    st1[0, 0:1] = mean
    st1[0, 1:2] = second
    rounds = chips // 2 - 1
    for k in range(rounds):
        pl.semaphore_wait(heard.at[k], len(near))
        if k + 1 < rounds:
            greet(heard.at[k + 1])
    for k in farthest:
        if k % 2 == 0:
            alike_copy(k).start()

    gets[2].wait()
    gets[3].wait()
    wv_v[...] = dot(wv_v[...], wo_v[...]).astype(BF16)

    def comm(r):
        for d in range(2):
            ref = piece(d, r, core)
            ring_copy(d, ref, r).wait_recv()

            @pl.when(r < steps - parts)
            def _():
                ring_copy(d, ref, r + parts).start()

            @pl.when(r == steps - parts)
            def _():
                for k in range(ends):
                    ring_copy(d, last_on(d, k), steps + k).start()

            sib_copy(ref, d, r).start()

    def comm_last(k):
        for d in range(2):
            ref = last(d, k, core)
            ring_copy(d, ref, steps + k).wait_recv()
            sib_copy(ref, d, steps + k).start()

    comm(0)
    alike_all().wait_recv()
    alike_over().start()
    comm(1)
    alike_over().wait_recv()
    for g in get_vecs:
        g.wait()
    a1, b1, centre1 = affine(st1[:, 0], st1[:, 1], float(count), vec[0], vec[1])
    gets[0].wait()
    gets[1].wait()
    normed = (gathered[me].astype(F32) * a1 + b1).astype(BF16)
    queries = dot(normed, wq_v[...]).astype(BF16)
    q_v[...] = (dot_t(queries, wk_v[...]) * (a1 * (LOG2E / C**0.5))).astype(BF16)

    m_v[...] = jnp.full_like(m_v, -1e30)
    l_v[...] = jnp.zeros_like(l_v)
    acc_v[...] = jnp.zeros_like(acc_v)

    def wide(x, width):
        return jnp.concatenate([x] * (width // 128), axis=1)

    def attend(keys):
        width = keys.shape[0]
        halves = [pl.ds(i * (count // 2), count // 2) for i in range(2)]
        scores = [dot_t(q_v[h], keys) for h in halves]
        for h, s in zip(halves, scores):
            old = m_v[h]
            new = jnp.maximum(old, jnp.max(s, axis=1, keepdims=True))
            scale = jnp.exp2(old - new)
            p = jnp.exp2(s - wide(new, width)).astype(BF16)
            back = p.astype(F32)
            l_v[h] = l_v[h] * scale + sum(back[:, i : i + 128] for i in range(0, width, 128))
            acc_v[h] = acc_v[h] * wide(scale, C) + dot(p, keys)
            m_v[h] = new

    def pieces(r, c):
        return [piece(0, r, c)[...], piece(1, r, c)[...]]

    def compute(r):
        for d in range(2):
            sib_copy(piece(d, r, 1 - core), d, r).wait_recv()
        attend(jnp.concatenate(pieces(r, core) + pieces(r, 1 - core), axis=0))

    attend(gathered[me])
    sib_copy(gathered.at[sib], 0, steps + ends).wait_recv()
    attend(gathered[sib])
    lax.fori_loop(0, parts - 1, lambda r, carry: (compute(r), carry)[1], 0)

    def step(r, carry):
        compute(r - 1)
        comm(r)
        return carry

    lax.fori_loop(parts, steps, step, 0)
    compute(steps - 1)

    def lasts(k, c):
        return [last(d, k, c)[...] for d in range(2)]

    def wait_last(k):
        for d in range(2):
            sib_copy(last(d, k, 1 - core), d, steps + k).wait_recv()

    comm_last(0)
    comm_last(1)
    wait_last(0)
    attend(jnp.concatenate(lasts(0, core) + lasts(0, 1 - core), axis=0))
    comm_last(2)
    wait_last(1)
    attend(jnp.concatenate(lasts(1, core) + lasts(1, 1 - core) + lasts(2, core), axis=0))
    wait_last(2)
    attend(jnp.concatenate(lasts(2, 1 - core), axis=0))

    total = jnp.sum(l_v[...], axis=1, keepdims=True)
    attended = (acc_v[...] * (1.0 / total) * a1 + b1).astype(BF16)
    hidden = (gathered[me].astype(F32) + dot(attended, wv_v[...])).astype(BF16)
    hid_v[...] = hidden

    def halo_copy(i):
        rows = pl.ds(count - W, W) if i == 0 else pl.ds(0, W)
        peer = lax.rem(me + 1, n) if i == 0 else lax.rem(me + n - 1, n)
        return pltpu.make_async_remote_copy(
            src_ref=hid_v.at[rows],
            dst_ref=halo_v.at[i],
            send_sem=halo_send.at[i],
            recv_sem=halo_recv.at[i],
            device_id={"row": peer},
            device_id_type=MESH,
        )

    mean, second = shifted_stats(hidden.astype(F32), centre1, float(count))
    st2[0, 0:1] = mean
    st2[0, 1:2] = second
    for k in farthest:
        stats_copy(st2, 1, k).start()
    for i in range(2):
        halo_copy(i).start()
    for t in range(parts):
        for d in range(2):
            ring_copy(d, own_piece(d, t), t).wait_send()

    def drain(r, carry):
        for d in range(2):
            ref = piece(d, r, core)

            @pl.when(r < steps - parts)
            def _():
                ring_copy(d, ref, r + parts).wait_send()

            sib_copy(ref, d, r).wait_send()
        return carry

    lax.fori_loop(0, steps, drain, 0)
    for k in range(ends):
        for d in range(2):
            ring_copy(d, last_on(d, k), steps + k).wait_send()
            sib_copy(last(d, k, core), d, steps + k).wait_send()
    for g in get_taps:
        g.wait()
    stats_all(st2, 1).wait_recv()
    a2, b2, _ = affine(st2[:, 0], st2[:, 1], float(count), vec[2], vec[3])
    for i in range(2):
        halo_copy(i).wait_recv()

    col = lax.broadcasted_iota(jnp.int32, (W, C), 0)
    image_rows = count // W

    def activate(b):
        if b == 0:
            f = halo_v[0]
        elif b == image_rows + 1:
            f = halo_v[1]
        else:
            f = hid_v[pl.ds((b - 1) * W, W)]
        v = f.astype(F32) * a2 + b2
        v = v / (1.0 + jnp.exp(-v))
        if b == 0:
            v = jnp.where(me > 0, v, 0.0)
        elif b == image_rows + 1:
            v = jnp.where(me < n - 1, v, 0.0)
        act_v[pl.ds(b * W, W)] = v.astype(BF16)

    part = image_rows // 2

    def convolve(h):
        around = jnp.concatenate(
            [act_v[pl.ds((h * part + i) * W, part * W)] for i in range(3)], axis=1
        )
        return {tap: dot(around, wc_v[tap].reshape(3 * C, C)) for tap in (0, 2, 1)}

    def finish(h, taps):
        for b in range(part):
            rows = slice(b * W, (b + 1) * W)
            left = jnp.where(col == 0, 0.0, pltpu.roll(taps[0][rows], 1, 0))
            right = jnp.where(col == W - 1, 0.0, pltpu.roll(taps[2][rows], W - 1, 0))
            conv = (left + right) + taps[1][rows]
            here = pl.ds((h * part + b) * W, W)
            out[here] = (hid_v[here].astype(F32) + (conv + vec[4])).astype(BF16)

    for b in range(part + 2):
        activate(b)
    first = convolve(0)
    for b in range(part + 2, image_rows + 2):
        activate(b)
    second = convolve(1)
    finish(0, first)
    finish(1, second)

    own_to_sib.wait_send()
    alike_all().wait_send()
    alike_over().wait_send()
    stats_all(st2, 1).wait_send()
    for i in range(2):
        halo_copy(i).wait_send()


def local(n, latent, g1, s1, w_query, w_key, w_value, w_out, g2, s2, w_conv, bias):
    rows = latent.shape[0]
    count = rows * W
    parts = count // PIECE
    steps = (n // 4 - 1) * parts + len(LAST)
    dma = pltpu.SemaphoreType.DMA
    vm = pltpu.VMEM
    def stay(x):
        return pltpu.with_memory_space_constraint(x, pltpu.HBM)

    result = pl.pallas_call(
        functools.partial(kernel, n),
        name="block",
        out_shape=jax.ShapeDtypeStruct((count, C), BF16),
        in_specs=[pl.BlockSpec(memory_space=pl.ANY)] * 11,
        out_specs=pl.BlockSpec(memory_space=pltpu.VMEM),
        scratch_shapes=[
            vm((n, count, C), BF16),
            vm((5, 1, C), F32),
            vm((C, C), BF16),
            vm((C, C), BF16),
            vm((C, C), BF16),
            vm((C, C), BF16),
            vm((3, 3, C, C), BF16),
            vm((count, C), BF16),
            vm((count, 128), F32),
            vm((count, 128), F32),
            vm((count, C), F32),
            vm((count, C), BF16),
            vm((2, W, C), BF16),
            vm((count + 2 * W, C), BF16),
            vm((n, 2, 128), F32),
            vm((n, 2, 128), F32),
            dma((15,)),
            dma((2, steps)),
            dma((2, steps)),
            dma((2, steps + 1)),
            dma((2, steps + 1)),
            pltpu.SemaphoreType.REGULAR((n // 4 - 1,)),
            dma((3,)),
            dma((3,)),
            dma((2,)),
            dma((2,)),
        ],
        compiler_params=pltpu.CompilerParams(
            collective_id=0, has_side_effects=True, vmem_limit_bytes=40 * 1024 * 1024
        ),
    )(
        stay(latent.reshape(count, C)),
        *(stay(v.reshape(1, C)) for v in (g1, s1, g2, s2, bias)),
        stay(w_query),
        stay(w_key),
        stay(w_value),
        stay(w_out),
        stay(w_conv),
    )
    return result.reshape(rows, W, C)


def solution(mesh):
    n = mesh.shape["row"]
    in_specs = (P(("img", "row"), None, None), P(), P(), P(), P(), P(), P(), P(), P(), P(), P())
    return jax.shard_map(
        functools.partial(local, n),
        mesh=mesh,
        in_specs=in_specs,
        out_specs=P(("img", "row"), None, None),
        check_vma=False,
    )
```

```python
import functools

import jax
import jax.numpy as jnp
from jax import lax
from jax.experimental import pallas as pl
from jax.experimental.pallas import tpu as pltpu
from jax.sharding import PartitionSpec as P

MESH = pl.DeviceIdType.MESH
C = 512
GROUP = 16
W = 128
EPS = 1e-06
PIECE = 256
LAST = (128, 64, 64)
LOG2E = 1.4426950408889634
F32 = jnp.float32
BF16 = jnp.bfloat16


def group_total(x):
    lane = lax.broadcasted_iota(jnp.int32, x.shape, 1)
    width = x.shape[1]
    for s in (1, 2, 4, 8):
        up = pltpu.roll(x, s, 1)
        down = pltpu.roll(x, width - s, 1)
        x = x + jnp.where((lane // s) % 2 == 1, up, down)
    return x


def channel_stats(x):
    mean = jnp.sum(x, axis=0, keepdims=True) * (1.0 / x.shape[0])
    off = x - mean
    return mean, jnp.sum(off * off, axis=0, keepdims=True)


def tiles(row):
    at = lax.broadcasted_iota(jnp.int32, (8, 128), 0) % (C // 128)
    out = jnp.broadcast_to(row[:, :128], (8, 128))
    for k in range(1, C // 128):
        out = jnp.where(at == k, row[:, 128 * k : 128 * (k + 1)], out)
    return out


def line(x):
    lane = lax.broadcasted_iota(jnp.int32, (8, 128), 1) % GROUP
    at = lax.broadcasted_iota(jnp.int32, (8, 128), 0)
    return jnp.sum(jnp.where(lane == at, x, 0.0), axis=0, keepdims=True)


def group_stats(mean, second, count):
    mean, second = tiles(mean), tiles(second)
    centre = group_total(mean) * (1.0 / GROUP)
    off = mean - centre
    return line(centre), line(group_total(second + count * (off * off)))


def shifted_stats(x, near, count):
    off = x - near
    first = jnp.sum(off, axis=0, keepdims=True)
    second = jnp.sum(off * off, axis=0, keepdims=True)
    at = lax.broadcasted_iota(jnp.int32, (8, 128), 0)
    total = group_total(jnp.where(at < C // 128, tiles(first), tiles(second)))
    lane = lax.broadcasted_iota(jnp.int32, (8, 128), 1) % GROUP
    mine = jnp.where(lane == at % (C // 128), total, 0.0)
    first = jnp.sum(jnp.where(at < C // 128, mine, 0.0), axis=0, keepdims=True)
    second = jnp.sum(jnp.where(at < C // 128, 0.0, mine), axis=0, keepdims=True)
    offset = first * (1.0 / (GROUP * count))
    lanes = lax.broadcasted_iota(jnp.int32, (1, 128), 1) % GROUP
    base = near[:, :128]
    for k in range(1, C // 128):
        base = jnp.where(lanes == k, near[:, 128 * k : 128 * (k + 1)], base)
    return base + offset, jnp.maximum(second - first * offset, 0.0)


def affine(means, seconds, count, gain, shift):
    devices = means.shape[0]
    centre = jnp.sum(means, axis=0, keepdims=True) * (1.0 / devices)
    off = means - centre
    size = count * GROUP
    second = jnp.sum(seconds + size * (off * off), axis=0, keepdims=True)
    scale = lax.rsqrt(second * (1.0 / (devices * size)) + EPS)
    at = lax.broadcasted_iota(jnp.int32, (8, 128), 0)
    lane = lax.broadcasted_iota(jnp.int32, (8, 128), 1)
    both = jnp.where(at < C // 128, centre, scale)
    both = jnp.take_along_axis(both, lane // GROUP * GROUP + at % (C // 128), axis=1)
    centre, scale = (
        jnp.concatenate([both[k : k + 1] for k in range(first, first + C // 128)], axis=1)
        for first in (0, C // 128)
    )
    a = scale * gain
    return a, shift - centre * a, centre


def dot(x, y):
    return jnp.dot(x, y, preferred_element_type=F32)


def dot_t(x, y):
    return lax.dot_general(x, y, (((1,), (1,)), ((), ())), preferred_element_type=F32)


def kernel(
    n,
    lat,
    g1,
    s1,
    g2,
    s2,
    bias,
    wq,
    wk,
    wv,
    wo,
    wc,
    out,
    gathered,
    vec,
    wq_v,
    wk_v,
    wv_v,
    wo_v,
    wc_v,
    wd_v,
    q_v,
    m_v,
    l_v,
    acc_v,
    hid_v,
    halo_v,
    act_v,
    st1,
    st2,
    local_sem,
    ring_send,
    ring_recv,
    sib_send,
    sib_recv,
    heard,
    st_send,
    st_recv,
    halo_send,
    halo_recv,
):
    me = lax.axis_index("row")
    chips = n // 2
    z, core = me // 2, me % 2
    sib = me + 1 - 2 * core
    count = lat.shape[0]
    parts = count // PIECE
    half = chips // 2
    steps = (half - 1) * parts
    ends = len(LAST)
    assert parts == 2 and sum(LAST) == PIECE
    nexts = (
        lax.rem(z + 1, chips) * 2 + core,
        lax.rem(z + chips - 1, chips) * 2 + core,
    )
    near = (sib,) + nexts + tuple(peer + 1 - 2 * core for peer in nexts)

    get_lat = pltpu.make_async_copy(lat, gathered.at[me], local_sem.at[0])
    get_lat.start()
    def greet(semaphore):
        for peer in near:
            pl.semaphore_signal(semaphore, inc=1, device_id={"row": peer}, device_id_type=MESH)

    barrier = pltpu.get_barrier_semaphore()
    greet(barrier)
    pl.semaphore_wait(barrier, len(near))

    def place(d, r, c):
        hop = 1 + r // parts
        chip = lax.rem(z + chips - hop, chips) if d == 0 else lax.rem(z + hop, chips)
        j = lax.rem(r, parts) if d == 0 else lax.rem(r + parts // 2, parts)
        return chip * 2 + c, j * PIECE

    def piece(d, r, c):
        slot, at = place(d, r, c)
        return gathered.at[slot, pl.ds(pl.multiple_of(at, PIECE), PIECE)]

    def last(d, k, c):
        at = (PIECE if d else 0) + sum(LAST[:k])
        return gathered.at[lax.rem(z + half, chips) * 2 + c, pl.ds(at, LAST[k])]

    def last_on(d, k):
        at = (PIECE if d else 0) + sum(LAST[:k])
        hop = half - 1
        chip = lax.rem(z + chips - hop, chips) if d == 0 else lax.rem(z + hop, chips)
        return gathered.at[chip * 2 + core, pl.ds(at, LAST[k])]

    def ring_copy(d, ref, t):
        return pltpu.make_async_remote_copy(
            src_ref=ref,
            dst_ref=ref,
            send_sem=ring_send.at[d, t],
            recv_sem=ring_recv.at[d, t],
            device_id={"row": nexts[d]},
            device_id_type=MESH,
        )

    def sib_copy(ref, d, r):
        return pltpu.make_async_remote_copy(
            src_ref=ref,
            dst_ref=ref,
            send_sem=sib_send.at[d, r],
            recv_sem=sib_recv.at[d, r],
            device_id={"row": sib},
            device_id_type=MESH,
        )

    def own_piece(d, t):
        j = t if d == 0 else (t + parts // 2) % parts
        return gathered.at[me, pl.ds(j * PIECE, PIECE)]

    get_lat.wait()
    for t in range(parts):
        for d in range(2):
            ring_copy(d, own_piece(d, t), t).start()
    own_to_sib = sib_copy(gathered.at[me], 0, steps + ends)
    own_to_sib.start()
    greet(heard.at[0])
    gets = []
    get_vecs = []
    for i, a in enumerate((g1, s1, g2, s2, bias)):
        get_vecs.append(pltpu.make_async_copy(a, vec.at[i], local_sem.at[7 + i]))
        get_vecs[-1].start()
    for i, (a, b) in enumerate(((wq, wq_v), (wk, wk_v), (wv, wv_v), (wo, wo_v))):
        gets.append(pltpu.make_async_copy(a, b, local_sem.at[2 + i]))
        gets[-1].start()
    get_taps = [
        pltpu.make_async_copy(wc.at[:, tap], wc_v.at[tap], local_sem.at[12 + tap]) for tap in range(3)
    ]
    for g in get_taps:
        g.start()


    farthest = sorted(range(1, n), key=lambda k: abs(k - n // 2))

    def stats_copy(buf, which, k):
        return pltpu.make_async_remote_copy(
            src_ref=buf.at[0],
            dst_ref=buf.at[k],
            send_sem=st_send.at[which],
            recv_sem=st_recv.at[which],
            device_id={"row": lax.rem(me + k, n)},
            device_id_type=MESH,
        )

    def alike_copy(k):
        return pltpu.make_async_remote_copy(
            src_ref=st1.at[0],
            dst_ref=st1.at[k // 2],
            send_sem=st_send.at[0],
            recv_sem=st_recv.at[0],
            device_id={"row": lax.rem(me + k, n)},
            device_id_type=MESH,
        )

    def alike_all():
        some = st1.at[pl.ds(1, chips - 1)]
        return pltpu.make_async_remote_copy(
            src_ref=some,
            dst_ref=some,
            send_sem=st_send.at[0],
            recv_sem=st_recv.at[0],
            device_id={"row": sib},
            device_id_type=MESH,
        )

    def alike_over():
        return pltpu.make_async_remote_copy(
            src_ref=st1.at[pl.ds(0, chips)],
            dst_ref=st1.at[pl.ds(chips, chips)],
            send_sem=st_send.at[2],
            recv_sem=st_recv.at[2],
            device_id={"row": sib},
            device_id_type=MESH,
        )

    def stats_all(buf, which):
        return pltpu.make_async_remote_copy(
            src_ref=buf.at[pl.ds(1, n - 1)],
            dst_ref=buf.at[pl.ds(1, n - 1)],
            send_sem=st_send.at[which],
            recv_sem=st_recv.at[which],
            device_id={"row": sib},
            device_id_type=MESH,
        )

    mean, second = channel_stats(gathered[me].astype(F32))
    mean, second = group_stats(mean, second, float(count))
    st1[0, 0:1] = mean
    st1[0, 1:2] = second
    rounds = chips // 2 - 1
    for k in range(rounds):
        pl.semaphore_wait(heard.at[k], len(near))
        if k + 1 < rounds:
            greet(heard.at[k + 1])
    for k in farthest:
        if k % 2 == 0:
            alike_copy(k).start()

    gets[2].wait()
    gets[3].wait()
    wv_v[...] = dot(wv_v[...], wo_v[...]).astype(BF16)

    def comm(r):
        for d in range(2):
            ref = piece(d, r, core)
            ring_copy(d, ref, r).wait_recv()

            @pl.when(r < steps - parts)
            def _():
                ring_copy(d, ref, r + parts).start()

            @pl.when(r == steps - parts)
            def _():
                for k in range(ends):
                    ring_copy(d, last_on(d, k), steps + k).start()

            sib_copy(ref, d, r).start()

    def comm_last(k):
        for d in range(2):
            ref = last(d, k, core)
            ring_copy(d, ref, steps + k).wait_recv()
            sib_copy(ref, d, steps + k).start()

    comm(0)
    alike_all().wait_recv()
    alike_over().start()
    comm(1)
    alike_over().wait_recv()
    for g in get_vecs:
        g.wait()
    a1, b1, centre1 = affine(st1[:, 0], st1[:, 1], float(count), vec[0], vec[1])
    gets[0].wait()
    gets[1].wait()
    normed = (gathered[me].astype(F32) * a1 + b1).astype(BF16)
    queries = dot(normed, wq_v[...]).astype(BF16)
    q_v[...] = (dot_t(queries, wk_v[...]) * (a1 * (LOG2E / C**0.5))).astype(BF16)

    m_v[...] = jnp.full_like(m_v, -1e30)
    l_v[...] = jnp.zeros_like(l_v)
    acc_v[...] = jnp.zeros_like(acc_v)

    def wide(x, width):
        return jnp.concatenate([x] * (width // 128), axis=1)

    def attend(keys):
        width = keys.shape[0]
        halves = [pl.ds(i * (count // 2), count // 2) for i in range(2)]
        scores = [dot_t(q_v[h], keys) for h in halves]
        for h, s in zip(halves, scores):
            old = m_v[h]
            new = jnp.maximum(old, jnp.max(s, axis=1, keepdims=True))
            scale = jnp.exp2(old - new)
            p = jnp.exp2(s - wide(new, width)).astype(BF16)
            back = p.astype(F32)
            l_v[h] = l_v[h] * scale + sum(back[:, i : i + 128] for i in range(0, width, 128))
            acc_v[h] = acc_v[h] * wide(scale, C) + dot(p, keys)
            m_v[h] = new

    def pieces(r, c):
        return [piece(0, r, c)[...], piece(1, r, c)[...]]

    def compute(r):
        for d in range(2):
            sib_copy(piece(d, r, 1 - core), d, r).wait_recv()
        attend(jnp.concatenate(pieces(r, core) + pieces(r, 1 - core), axis=0))

    attend(gathered[me])
    sib_copy(gathered.at[sib], 0, steps + ends).wait_recv()
    attend(gathered[sib])

    for g in get_taps:
        g.wait()
    for tap in range(3):
        ends_of = wc_v[tap, 0].astype(F32) + wc_v[tap, 2].astype(F32)
        middle = wc_v[tap, 1].astype(F32)
        wc_v[tap, 1] = ((ends_of + middle) * 0.5).astype(BF16)
        wd_v[tap] = ((ends_of - middle) * 0.5).astype(BF16)
    lax.fori_loop(0, parts - 1, lambda r, carry: (compute(r), carry)[1], 0)

    def step(r, carry):
        compute(r - 1)
        comm(r)
        return carry

    lax.fori_loop(parts, steps, step, 0)
    compute(steps - 1)

    def lasts(k, c):
        return [last(d, k, c)[...] for d in range(2)]

    def wait_last(k):
        for d in range(2):
            sib_copy(last(d, k, 1 - core), d, steps + k).wait_recv()

    comm_last(0)
    comm_last(1)
    wait_last(0)
    attend(jnp.concatenate(lasts(0, core) + lasts(0, 1 - core), axis=0))
    comm_last(2)
    wait_last(1)
    attend(jnp.concatenate(lasts(1, core) + lasts(1, 1 - core) + lasts(2, core), axis=0))
    wait_last(2)
    attend(jnp.concatenate(lasts(2, 1 - core), axis=0))

    total = jnp.sum(l_v[...], axis=1, keepdims=True)
    attended = (acc_v[...] * (1.0 / total) * a1 + b1).astype(BF16)
    hidden = (gathered[me].astype(F32) + dot(attended, wv_v[...])).astype(BF16)
    hid_v[...] = hidden

    def halo_copy(i):
        rows = pl.ds(count - W, W) if i == 0 else pl.ds(0, W)
        peer = lax.rem(me + 1, n) if i == 0 else lax.rem(me + n - 1, n)
        return pltpu.make_async_remote_copy(
            src_ref=hid_v.at[rows],
            dst_ref=halo_v.at[i],
            send_sem=halo_send.at[i],
            recv_sem=halo_recv.at[i],
            device_id={"row": peer},
            device_id_type=MESH,
        )

    mean, second = shifted_stats(hidden.astype(F32), centre1, float(count))
    st2[0, 0:1] = mean
    st2[0, 1:2] = second
    for k in farthest:
        stats_copy(st2, 1, k).start()
    for i in range(2):
        halo_copy(i).start()
    for t in range(parts):
        for d in range(2):
            ring_copy(d, own_piece(d, t), t).wait_send()

    def drain(r, carry):
        for d in range(2):
            ref = piece(d, r, core)

            @pl.when(r < steps - parts)
            def _():
                ring_copy(d, ref, r + parts).wait_send()

            sib_copy(ref, d, r).wait_send()
        return carry

    lax.fori_loop(0, steps, drain, 0)
    for k in range(ends):
        for d in range(2):
            ring_copy(d, last_on(d, k), steps + k).wait_send()
            sib_copy(last(d, k, core), d, steps + k).wait_send()
    stats_all(st2, 1).wait_recv()
    a2, b2, _ = affine(st2[:, 0], st2[:, 1], float(count), vec[2], vec[3])
    for i in range(2):
        halo_copy(i).wait_recv()

    col = lax.broadcasted_iota(jnp.int32, (W, C), 0)
    image_rows = count // W

    def activate(b):
        if b == 0:
            f = halo_v[0]
        elif b == image_rows + 1:
            f = halo_v[1]
        else:
            f = hid_v[pl.ds((b - 1) * W, W)]
        v = f.astype(F32) * a2 + b2
        v = v / (1.0 + jnp.exp(-v))
        if b == 0:
            v = jnp.where(me > 0, v, 0.0)
        elif b == image_rows + 1:
            v = jnp.where(me < n - 1, v, 0.0)
        act_v[pl.ds(b * W, W)] = v.astype(BF16)

    for b in range(image_rows + 2):
        activate(b)

    def row(b):
        return act_v[pl.ds(b * W, W)].astype(F32)

    pairs = range(0, image_rows, 2)

    def product(make, weights):
        left = jnp.concatenate([make(b).astype(BF16) for b in pairs], axis=0)
        return dot(left, jnp.concatenate(weights, axis=1))

    p1 = product(lambda b: row(b + 1) + row(b + 2), [wc_v[tap, 1] for tap in range(3)])
    p2 = product(lambda b: row(b + 2) - row(b + 1), [wd_v[tap] for tap in range(3)])
    p0 = product(lambda b: row(b) - row(b + 2), [wc_v[tap, 0] for tap in range(3)])
    p3 = product(lambda b: row(b + 1) - row(b + 3), [wc_v[tap, 2] for tap in range(3)])

    def finish(b, taps):
        left = jnp.where(col == 0, 0.0, pltpu.roll(taps[:, :C], 1, 0))
        right = jnp.where(col == W - 1, 0.0, pltpu.roll(taps[:, 2 * C :], W - 1, 0))
        conv = (left + right) + taps[:, C : 2 * C]
        here = pl.ds(b * W, W)
        out[here] = (hid_v[here].astype(F32) + (conv + vec[4])).astype(BF16)

    for k, b in enumerate(pairs):
        rows = slice(k * W, (k + 1) * W)
        finish(b, p1[rows] + p2[rows] + p0[rows])
    for k, b in enumerate(pairs):
        rows = slice(k * W, (k + 1) * W)
        finish(b + 1, p1[rows] - p2[rows] - p3[rows])

    own_to_sib.wait_send()
    alike_all().wait_send()
    alike_over().wait_send()
    stats_all(st2, 1).wait_send()
    for i in range(2):
        halo_copy(i).wait_send()


def local(n, latent, g1, s1, w_query, w_key, w_value, w_out, g2, s2, w_conv, bias):
    rows = latent.shape[0]
    count = rows * W
    parts = count // PIECE
    steps = (n // 4 - 1) * parts + len(LAST)
    dma = pltpu.SemaphoreType.DMA
    vm = pltpu.VMEM
    def stay(x):
        return pltpu.with_memory_space_constraint(x, pltpu.HBM)

    result = pl.pallas_call(
        functools.partial(kernel, n),
        name="block",
        out_shape=jax.ShapeDtypeStruct((count, C), BF16),
        in_specs=[pl.BlockSpec(memory_space=pl.ANY)] * 11,
        out_specs=pl.BlockSpec(memory_space=pltpu.VMEM),
        scratch_shapes=[
            vm((n, count, C), BF16),
            vm((5, 1, C), F32),
            vm((C, C), BF16),
            vm((C, C), BF16),
            vm((C, C), BF16),
            vm((C, C), BF16),
            vm((3, 3, C, C), BF16),
            vm((3, C, C), BF16),
            vm((count, C), BF16),
            vm((count, 128), F32),
            vm((count, 128), F32),
            vm((count, C), F32),
            vm((count, C), BF16),
            vm((2, W, C), BF16),
            vm((count + 2 * W, C), BF16),
            vm((n, 2, 128), F32),
            vm((n, 2, 128), F32),
            dma((15,)),
            dma((2, steps)),
            dma((2, steps)),
            dma((2, steps + 1)),
            dma((2, steps + 1)),
            pltpu.SemaphoreType.REGULAR((n // 4 - 1,)),
            dma((3,)),
            dma((3,)),
            dma((2,)),
            dma((2,)),
        ],
        compiler_params=pltpu.CompilerParams(
            collective_id=0, has_side_effects=True, vmem_limit_bytes=40 * 1024 * 1024
        ),
    )(
        stay(latent.reshape(count, C)),
        *(stay(v.reshape(1, C)) for v in (g1, s1, g2, s2, bias)),
        stay(w_query),
        stay(w_key),
        stay(w_value),
        stay(w_out),
        stay(w_conv),
    )
    return result.reshape(rows, W, C)


def solution(mesh):
    n = mesh.shape["row"]
    in_specs = (P(("img", "row"), None, None), P(), P(), P(), P(), P(), P(), P(), P(), P(), P())
    return jax.shard_map(
        functools.partial(local, n),
        mesh=mesh,
        in_specs=in_specs,
        out_specs=P(("img", "row"), None, None),
        check_vma=False,
    )
```

```python
import functools

import jax
import jax.numpy as jnp
from jax import lax
from jax.experimental import pallas as pl
from jax.experimental.pallas import tpu as pltpu
from jax.sharding import PartitionSpec as P

MESH = pl.DeviceIdType.MESH
C = 512
GROUP = 16
W = 128
EPS = 1e-06
PIECE = 256
LAST = (128, 64, 64)
LOG2E = 1.4426950408889634
F32 = jnp.float32
BF16 = jnp.bfloat16


def group_total(x):
    lane = lax.broadcasted_iota(jnp.int32, x.shape, 1)
    width = x.shape[1]
    for s in (1, 2, 4, 8):
        up = pltpu.roll(x, s, 1)
        down = pltpu.roll(x, width - s, 1)
        x = x + jnp.where((lane // s) % 2 == 1, up, down)
    return x


def channel_stats(x):
    mean = jnp.sum(x, axis=0, keepdims=True) * (1.0 / x.shape[0])
    off = x - mean
    return mean, jnp.sum(off * off, axis=0, keepdims=True)


def tiles(row):
    at = lax.broadcasted_iota(jnp.int32, (8, 128), 0) % (C // 128)
    out = jnp.broadcast_to(row[:, :128], (8, 128))
    for k in range(1, C // 128):
        out = jnp.where(at == k, row[:, 128 * k : 128 * (k + 1)], out)
    return out


def line(x):
    lane = lax.broadcasted_iota(jnp.int32, (8, 128), 1) % GROUP
    at = lax.broadcasted_iota(jnp.int32, (8, 128), 0)
    return jnp.sum(jnp.where(lane == at, x, 0.0), axis=0, keepdims=True)


def group_stats(mean, second, count):
    mean, second = tiles(mean), tiles(second)
    centre = group_total(mean) * (1.0 / GROUP)
    off = mean - centre
    return line(centre), line(group_total(second + count * (off * off)))


def shifted_stats(x, near, count):
    off = x - near
    first = jnp.sum(off, axis=0, keepdims=True)
    second = jnp.sum(off * off, axis=0, keepdims=True)
    at = lax.broadcasted_iota(jnp.int32, (8, 128), 0)
    total = group_total(jnp.where(at < C // 128, tiles(first), tiles(second)))
    lane = lax.broadcasted_iota(jnp.int32, (8, 128), 1) % GROUP
    mine = jnp.where(lane == at % (C // 128), total, 0.0)
    first = jnp.sum(jnp.where(at < C // 128, mine, 0.0), axis=0, keepdims=True)
    second = jnp.sum(jnp.where(at < C // 128, 0.0, mine), axis=0, keepdims=True)
    offset = first * (1.0 / (GROUP * count))
    lanes = lax.broadcasted_iota(jnp.int32, (1, 128), 1) % GROUP
    base = near[:, :128]
    for k in range(1, C // 128):
        base = jnp.where(lanes == k, near[:, 128 * k : 128 * (k + 1)], base)
    return base + offset, jnp.maximum(second - first * offset, 0.0)


def affine(means, seconds, count, gain, shift):
    devices = means.shape[0]
    centre = jnp.sum(means, axis=0, keepdims=True) * (1.0 / devices)
    off = means - centre
    size = count * GROUP
    second = jnp.sum(seconds + size * (off * off), axis=0, keepdims=True)
    scale = lax.rsqrt(second * (1.0 / (devices * size)) + EPS)
    at = lax.broadcasted_iota(jnp.int32, (8, 128), 0)
    lane = lax.broadcasted_iota(jnp.int32, (8, 128), 1)
    both = jnp.where(at < C // 128, centre, scale)
    both = jnp.take_along_axis(both, lane // GROUP * GROUP + at % (C // 128), axis=1)
    centre, scale = (
        jnp.concatenate([both[k : k + 1] for k in range(first, first + C // 128)], axis=1)
        for first in (0, C // 128)
    )
    a = scale * gain
    return a, shift - centre * a, centre


def dot(x, y):
    return jnp.dot(x, y, preferred_element_type=F32)


def dot_t(x, y):
    return lax.dot_general(x, y, (((1,), (1,)), ((), ())), preferred_element_type=F32)


def kernel(
    n,
    lat,
    g1,
    s1,
    g2,
    s2,
    bias,
    wq,
    wk,
    wv,
    wo,
    wc,
    out,
    gathered,
    vec,
    wq_v,
    wk_v,
    wv_v,
    wo_v,
    wc_v,
    wd_v,
    q_v,
    m_v,
    l_v,
    acc_v,
    hid_v,
    halo_v,
    act_v,
    st1,
    st2,
    local_sem,
    ring_send,
    ring_recv,
    sib_send,
    sib_recv,
    heard,
    st_send,
    st_recv,
    halo_send,
    halo_recv,
):
    me = lax.axis_index("row")
    chips = n // 2
    z, core = me // 2, me % 2
    sib = me + 1 - 2 * core
    count = lat.shape[0]
    parts = count // PIECE
    half = chips // 2
    steps = (half - 1) * parts
    ends = len(LAST)
    assert parts == 2 and sum(LAST) == PIECE
    nexts = (
        lax.rem(z + 1, chips) * 2 + core,
        lax.rem(z + chips - 1, chips) * 2 + core,
    )
    near = (sib,) + nexts + tuple(peer + 1 - 2 * core for peer in nexts)

    get_lat = pltpu.make_async_copy(lat, gathered.at[me], local_sem.at[0])
    get_lat.start()
    def greet(semaphore):
        for peer in near:
            pl.semaphore_signal(semaphore, inc=1, device_id={"row": peer}, device_id_type=MESH)

    barrier = pltpu.get_barrier_semaphore()
    greet(barrier)
    pl.semaphore_wait(barrier, len(near))

    def place(d, r, c):
        hop = 1 + r // parts
        chip = lax.rem(z + chips - hop, chips) if d == 0 else lax.rem(z + hop, chips)
        j = lax.rem(r, parts) if d == 0 else lax.rem(r + parts // 2, parts)
        return chip * 2 + c, j * PIECE

    def piece(d, r, c):
        slot, at = place(d, r, c)
        return gathered.at[slot, pl.ds(pl.multiple_of(at, PIECE), PIECE)]

    def last(d, k, c):
        at = (PIECE if d else 0) + sum(LAST[:k])
        return gathered.at[lax.rem(z + half, chips) * 2 + c, pl.ds(at, LAST[k])]

    def last_on(d, k):
        at = (PIECE if d else 0) + sum(LAST[:k])
        hop = half - 1
        chip = lax.rem(z + chips - hop, chips) if d == 0 else lax.rem(z + hop, chips)
        return gathered.at[chip * 2 + core, pl.ds(at, LAST[k])]

    def ring_copy(d, ref, t):
        return pltpu.make_async_remote_copy(
            src_ref=ref,
            dst_ref=ref,
            send_sem=ring_send.at[d, t],
            recv_sem=ring_recv.at[d, t],
            device_id={"row": nexts[d]},
            device_id_type=MESH,
        )

    def sib_copy(ref, d, r):
        return pltpu.make_async_remote_copy(
            src_ref=ref,
            dst_ref=ref,
            send_sem=sib_send.at[d, r],
            recv_sem=sib_recv.at[d, r],
            device_id={"row": sib},
            device_id_type=MESH,
        )

    def own_piece(d, t):
        j = t if d == 0 else (t + parts // 2) % parts
        return gathered.at[me, pl.ds(j * PIECE, PIECE)]

    get_lat.wait()
    for t in range(parts):
        for d in range(2):
            ring_copy(d, own_piece(d, t), t).start()
    own_to_sib = sib_copy(gathered.at[me], 0, steps + ends)
    own_to_sib.start()
    greet(heard.at[0])
    gets = []
    get_vecs = []
    for i, a in enumerate((g1, s1, g2, s2, bias)):
        get_vecs.append(pltpu.make_async_copy(a, vec.at[i], local_sem.at[7 + i]))
        get_vecs[-1].start()
    for i, (a, b) in enumerate(((wq, wq_v), (wk, wk_v), (wv, wv_v), (wo, wo_v))):
        gets.append(pltpu.make_async_copy(a, b, local_sem.at[2 + i]))
        gets[-1].start()
    get_taps = [
        pltpu.make_async_copy(wc.at[:, tap], wc_v.at[tap], local_sem.at[12 + tap]) for tap in range(3)
    ]
    for g in get_taps:
        g.start()


    farthest = sorted(range(1, n), key=lambda k: abs(k - n // 2))

    def stats_copy(buf, which, k):
        return pltpu.make_async_remote_copy(
            src_ref=buf.at[0],
            dst_ref=buf.at[k],
            send_sem=st_send.at[which],
            recv_sem=st_recv.at[which],
            device_id={"row": lax.rem(me + k, n)},
            device_id_type=MESH,
        )

    def alike_copy(k):
        return pltpu.make_async_remote_copy(
            src_ref=st1.at[0],
            dst_ref=st1.at[k // 2],
            send_sem=st_send.at[0],
            recv_sem=st_recv.at[0],
            device_id={"row": lax.rem(me + k, n)},
            device_id_type=MESH,
        )

    def alike_all():
        some = st1.at[pl.ds(1, chips - 1)]
        return pltpu.make_async_remote_copy(
            src_ref=some,
            dst_ref=some,
            send_sem=st_send.at[0],
            recv_sem=st_recv.at[0],
            device_id={"row": sib},
            device_id_type=MESH,
        )

    def alike_over():
        return pltpu.make_async_remote_copy(
            src_ref=st1.at[pl.ds(0, chips)],
            dst_ref=st1.at[pl.ds(chips, chips)],
            send_sem=st_send.at[2],
            recv_sem=st_recv.at[2],
            device_id={"row": sib},
            device_id_type=MESH,
        )

    def stats_all(buf, which):
        return pltpu.make_async_remote_copy(
            src_ref=buf.at[pl.ds(1, n - 1)],
            dst_ref=buf.at[pl.ds(1, n - 1)],
            send_sem=st_send.at[which],
            recv_sem=st_recv.at[which],
            device_id={"row": sib},
            device_id_type=MESH,
        )

    mean, second = channel_stats(gathered[me].astype(F32))
    mean, second = group_stats(mean, second, float(count))
    st1[0, 0:1] = mean
    st1[0, 1:2] = second
    rounds = chips // 2 - 1
    for k in range(rounds):
        pl.semaphore_wait(heard.at[k], len(near))
        if k + 1 < rounds:
            greet(heard.at[k + 1])
    for k in farthest:
        if k % 2 == 0:
            alike_copy(k).start()

    gets[2].wait()
    gets[3].wait()
    wv_v[...] = dot(wv_v[...], wo_v[...]).astype(BF16)

    def comm(r):
        for d in range(2):
            ref = piece(d, r, core)
            ring_copy(d, ref, r).wait_recv()

            @pl.when(r < steps - parts)
            def _():
                ring_copy(d, ref, r + parts).start()

            @pl.when(r == steps - parts)
            def _():
                for k in range(ends):
                    ring_copy(d, last_on(d, k), steps + k).start()

            sib_copy(ref, d, r).start()

    def comm_last(k):
        for d in range(2):
            ref = last(d, k, core)
            ring_copy(d, ref, steps + k).wait_recv()
            sib_copy(ref, d, steps + k).start()

    comm(0)
    alike_all().wait_recv()
    alike_over().start()
    comm(1)
    alike_over().wait_recv()
    for g in get_vecs:
        g.wait()
    a1, b1, centre1 = affine(st1[:, 0], st1[:, 1], float(count), vec[0], vec[1])
    gets[0].wait()
    gets[1].wait()
    normed = (gathered[me].astype(F32) * a1 + b1).astype(BF16)
    queries = dot(normed, wq_v[...]).astype(BF16)
    q_v[...] = (dot_t(queries, wk_v[...]) * (a1 * (LOG2E / C**0.5))).astype(BF16)

    m_v[...] = jnp.full_like(m_v, -1e30)
    l_v[...] = jnp.zeros_like(l_v)
    acc_v[...] = jnp.zeros_like(acc_v)

    def wide(x, width):
        return jnp.concatenate([x] * (width // 128), axis=1)

    def attend(keys):
        width = keys.shape[0]
        halves = [pl.ds(i * (count // 2), count // 2) for i in range(2)]
        scores = [dot_t(q_v[h], keys) for h in halves]
        for h, s in zip(halves, scores):
            old = m_v[h]
            new = jnp.maximum(old, jnp.max(s, axis=1, keepdims=True))
            scale = jnp.exp2(old - new)
            p = jnp.exp2(s - wide(new, width)).astype(BF16)
            back = p.astype(F32)
            l_v[h] = l_v[h] * scale + sum(back[:, i : i + 128] for i in range(0, width, 128))
            acc_v[h] = acc_v[h] * wide(scale, C) + dot(p, keys)
            m_v[h] = new

    def pieces(r, c):
        return [piece(0, r, c)[...], piece(1, r, c)[...]]

    def compute(r):
        for d in range(2):
            sib_copy(piece(d, r, 1 - core), d, r).wait_recv()
        attend(jnp.concatenate(pieces(r, core) + pieces(r, 1 - core), axis=0))

    attend(gathered[me])
    sib_copy(gathered.at[sib], 0, steps + ends).wait_recv()
    attend(gathered[sib])

    for g in get_taps:
        g.wait()
    for tap in range(3):
        ends_of = wc_v[tap, 0].astype(F32) + wc_v[tap, 2].astype(F32)
        middle = wc_v[tap, 1].astype(F32)
        wc_v[tap, 1] = ((ends_of + middle) * 0.5).astype(BF16)
        wd_v[tap] = ((ends_of - middle) * 0.5).astype(BF16)
    lax.fori_loop(0, parts - 1, lambda r, carry: (compute(r), carry)[1], 0)

    def step(r, carry):
        compute(r - 1)
        comm(r)
        return carry

    lax.fori_loop(parts, steps, step, 0)
    compute(steps - 1)

    def lasts(k, c):
        return [last(d, k, c)[...] for d in range(2)]

    def wait_last(k):
        for d in range(2):
            sib_copy(last(d, k, 1 - core), d, steps + k).wait_recv()

    comm_last(0)
    comm_last(1)
    wait_last(0)
    attend(jnp.concatenate(lasts(0, core) + lasts(0, 1 - core), axis=0))
    comm_last(2)
    wait_last(1)
    attend(jnp.concatenate(lasts(1, core) + lasts(1, 1 - core) + lasts(2, core), axis=0))
    wait_last(2)
    attend(jnp.concatenate(lasts(2, 1 - core), axis=0))

    total = jnp.sum(l_v[...], axis=1, keepdims=True)
    attended = (acc_v[...] * (1.0 / total) * a1 + b1).astype(BF16)
    hidden = (gathered[me].astype(F32) + dot(attended, wv_v[...])).astype(BF16)
    hid_v[...] = hidden

    def halo_copy(i):
        rows = pl.ds(count - W, W) if i == 0 else pl.ds(0, W)
        peer = lax.rem(me + 1, n) if i == 0 else lax.rem(me + n - 1, n)
        return pltpu.make_async_remote_copy(
            src_ref=hid_v.at[rows],
            dst_ref=halo_v.at[i],
            send_sem=halo_send.at[i],
            recv_sem=halo_recv.at[i],
            device_id={"row": peer},
            device_id_type=MESH,
        )

    mean, second = shifted_stats(hidden.astype(F32), centre1, float(count))
    st2[0, 0:1] = mean
    st2[0, 1:2] = second
    for k in farthest:
        stats_copy(st2, 1, k).start()
    for i in range(2):
        halo_copy(i).start()
    for t in range(parts):
        for d in range(2):
            ring_copy(d, own_piece(d, t), t).wait_send()

    def drain(r, carry):
        for d in range(2):
            ref = piece(d, r, core)

            @pl.when(r < steps - parts)
            def _():
                ring_copy(d, ref, r + parts).wait_send()

            sib_copy(ref, d, r).wait_send()
        return carry

    lax.fori_loop(0, steps, drain, 0)
    for k in range(ends):
        for d in range(2):
            ring_copy(d, last_on(d, k), steps + k).wait_send()
            sib_copy(last(d, k, core), d, steps + k).wait_send()
    stats_all(st2, 1).wait_recv()
    a2, b2, _ = affine(st2[:, 0], st2[:, 1], float(count), vec[2], vec[3])

    col = lax.broadcasted_iota(jnp.int32, (W, C), 0)
    image_rows = count // W

    def activate(b):
        if b == 0:
            f = halo_v[0]
        elif b == image_rows + 1:
            f = halo_v[1]
        else:
            f = hid_v[pl.ds((b - 1) * W, W)]
        v = f.astype(F32) * a2 + b2
        v = v / (1.0 + jnp.exp(-v))
        if b == 0:
            v = jnp.where(me > 0, v, 0.0)
        elif b == image_rows + 1:
            v = jnp.where(me < n - 1, v, 0.0)
        act_v[pl.ds(b * W, W)] = v.astype(BF16)

    for b in range(1, image_rows + 1):
        activate(b)

    def row(b):
        return act_v[pl.ds(b * W, W)].astype(F32)

    pairs = range(0, image_rows, 2)

    def product(make, weights):
        left = jnp.concatenate([make(b).astype(BF16) for b in pairs], axis=0)
        return dot(left, jnp.concatenate(weights, axis=1))

    p1 = product(lambda b: row(b + 1) + row(b + 2), [wc_v[tap, 1] for tap in range(3)])
    p2 = product(lambda b: row(b + 2) - row(b + 1), [wd_v[tap] for tap in range(3)])
    for i in range(2):
        halo_copy(i).wait_recv()
    activate(0)
    activate(image_rows + 1)
    p0 = product(lambda b: row(b) - row(b + 2), [wc_v[tap, 0] for tap in range(3)])
    p3 = product(lambda b: row(b + 1) - row(b + 3), [wc_v[tap, 2] for tap in range(3)])

    def finish(b, taps):
        left = jnp.where(col == 0, 0.0, pltpu.roll(taps[:, :C], 1, 0))
        right = jnp.where(col == W - 1, 0.0, pltpu.roll(taps[:, 2 * C :], W - 1, 0))
        conv = (left + right) + taps[:, C : 2 * C]
        here = pl.ds(b * W, W)
        out[here] = (hid_v[here].astype(F32) + (conv + vec[4])).astype(BF16)

    for k, b in enumerate(pairs):
        rows = slice(k * W, (k + 1) * W)
        finish(b, p1[rows] + p2[rows] + p0[rows])
    for k, b in enumerate(pairs):
        rows = slice(k * W, (k + 1) * W)
        finish(b + 1, p1[rows] - p2[rows] - p3[rows])

    own_to_sib.wait_send()
    alike_all().wait_send()
    alike_over().wait_send()
    stats_all(st2, 1).wait_send()
    for i in range(2):
        halo_copy(i).wait_send()


def local(n, latent, g1, s1, w_query, w_key, w_value, w_out, g2, s2, w_conv, bias):
    rows = latent.shape[0]
    count = rows * W
    parts = count // PIECE
    steps = (n // 4 - 1) * parts + len(LAST)
    dma = pltpu.SemaphoreType.DMA
    vm = pltpu.VMEM
    def stay(x):
        return pltpu.with_memory_space_constraint(x, pltpu.HBM)

    result = pl.pallas_call(
        functools.partial(kernel, n),
        name="block",
        out_shape=jax.ShapeDtypeStruct((count, C), BF16),
        in_specs=[pl.BlockSpec(memory_space=pl.ANY)] * 11,
        out_specs=pl.BlockSpec(memory_space=pltpu.VMEM),
        scratch_shapes=[
            vm((n, count, C), BF16),
            vm((5, 1, C), F32),
            vm((C, C), BF16),
            vm((C, C), BF16),
            vm((C, C), BF16),
            vm((C, C), BF16),
            vm((3, 3, C, C), BF16),
            vm((3, C, C), BF16),
            vm((count, C), BF16),
            vm((count, 128), F32),
            vm((count, 128), F32),
            vm((count, C), F32),
            vm((count, C), BF16),
            vm((2, W, C), BF16),
            vm((count + 2 * W, C), BF16),
            vm((n, 2, 128), F32),
            vm((n, 2, 128), F32),
            dma((15,)),
            dma((2, steps)),
            dma((2, steps)),
            dma((2, steps + 1)),
            dma((2, steps + 1)),
            pltpu.SemaphoreType.REGULAR((n // 4 - 1,)),
            dma((3,)),
            dma((3,)),
            dma((2,)),
            dma((2,)),
        ],
        compiler_params=pltpu.CompilerParams(
            collective_id=0, has_side_effects=True, vmem_limit_bytes=40 * 1024 * 1024
        ),
    )(
        stay(latent.reshape(count, C)),
        *(stay(v.reshape(1, C)) for v in (g1, s1, g2, s2, bias)),
        stay(w_query),
        stay(w_key),
        stay(w_value),
        stay(w_out),
        stay(w_conv),
    )
    return result.reshape(rows, W, C)


def solution(mesh):
    n = mesh.shape["row"]
    in_specs = (P(("img", "row"), None, None), P(), P(), P(), P(), P(), P(), P(), P(), P(), P())
    return jax.shard_map(
        functools.partial(local, n),
        mesh=mesh,
        in_specs=in_specs,
        out_specs=P(("img", "row"), None, None),
        check_vma=False,
    )
```
